32 devices in a mesh: section: 8 (over y, x, core), slab: 4 (over z).
Axes of the slice: x: 2, y: 2, z: 4, core: 2. Of those that a mesh axis runs over, the one named last changes fastest.
Arguments:
- emitted: bfloat16 [8, 20, 512, 512], P('section', None, 'slab'), may hold values from -6 to 6
- returned: bfloat16 [8, 20, 512, 512], P('section', None, 'slab'), may hold values from -6 to 6
- stash: bfloat16 [8, 20, 512, 512], P('section', None, 'slab'), may hold values from -6 to 6
- skip_w: bfloat16 [8, 2, 20, 20], P('section'), may hold values from -1.25 to 1.25
- up_w: bfloat16 [8, 2, 80, 20], P('section'), may hold values from -1.25 to 1.25
- down_w: bfloat16 [8, 2, 20, 80], P('section'), may hold values from -0.625 to 0.625
- spec_w: bfloat16 [8, 2, 64, 2, 20, 20, 128], P('section', None, 'slab'), may hold values from -4 to 4
Outputs:
- sent: bfloat16 [8, 20, 512, 512], P('section', None, 'slab')
- back_grad: bfloat16 [8, 20, 512, 512], P('section', None, 'slab')
- grad_skip: float32 [8, 2, 20, 20], P('section')
- grad_up: float32 [8, 2, 80, 20], P('section')
- grad_down: float32 [8, 2, 20, 80], P('section')
- grad_spec: float32 [8, 2, 64, 2, 20, 20, 128], P('section', None, 'slab')
The draws below stay inside these ranges and needn't reach their ends.
All inputs are finite; a program needn't handle non-finite values.
Results may differ from the reference program's by a relative error of at most 0.03.
Values may be sent and summed in bfloat16 or wider, within the bound.
A program may use at most 192 MiB of HBM per device.

```python
import jax
import jax.numpy as jnp
from jax import lax

N = 512
C = 20
F = 80
M = 64
LAYERS = 2
SECTIONS = 8


def block_scale(key, shape, cuts, low, high):
    def one(axis_at, shards_of):
        steps = jax.random.uniform(jax.random.fold_in(jax.random.fold_in(key, 6), axis_at), (shards_of,), jnp.float32, low / len(cuts), high / len(cuts))
        return jnp.repeat(jnp.exp(steps), shape[axis_at] // shards_of).reshape((-1,) + (1,) * (len(shape) - axis_at - 1))

    loudness = one(*cuts[0])
    for cut in cuts[1:]:
        loudness = loudness * one(*cut)
    return loudness


def normal_values(own_key, dims, spread, bound, cuts=(), kind=jnp.bfloat16):
    level = block_scale(own_key, dims, cuts, -0.22, 0.18) if cuts else 1.0
    array = jax.random.normal(own_key, dims, jnp.float32) * spread * level
    return jnp.minimum(jnp.maximum(array, -bound), bound).astype(kind)


def setup_inputs(seed: int = 0) -> dict:
    keys = jax.random.split(jax.random.key(seed), 8)
    return {
        "emitted": normal_values(keys[0], (SECTIONS, C, N, N), 1.0, 6.0, ((0, 8), (2, 4))),
        "returned": normal_values(keys[1], (SECTIONS, C, N, N), 1.0, 6.0, ((0, 8), (2, 4))),
        "stash": normal_values(keys[2], (SECTIONS, C, N, N), 1.0, 6.0, ((0, 8), (2, 4))),
        "skip_w": normal_values(keys[3], (SECTIONS, LAYERS, C, C), C ** -0.5, 1.25, ((0, 8),)),
        "up_w": normal_values(keys[4], (SECTIONS, LAYERS, F, C), C ** -0.5, 1.25, ((0, 8),)),
        "down_w": normal_values(keys[5], (SECTIONS, LAYERS, C, F), F ** -0.5, 0.625, ((0, 8),)),
        "spec_w": normal_values(keys[6], (SECTIONS, LAYERS, M, 2, C, C, 2 * M), 0.6, 4.0, ((0, 8), (2, 4))),
    }


root_two_pi = 0.7978845608028654
cubic_coef = 0.044715


def smooth_gate(values):
    return 0.5 * values * (1.0 + jnp.tanh(root_two_pi * (values + cubic_coef * values * values * values)))


def gate_slope(values):
    tangent = jnp.tanh(root_two_pi * (values + cubic_coef * values * values * values))
    return 0.5 * (1.0 + tangent) + 0.5 * values * (1.0 - tangent * tangent) * root_two_pi * (1.0 + 3.0 * cubic_coef * values * values)


def angles(left_idx, right_idx, length):
    product_idx = (left_idx[:, None] * right_idx[None, :]) % length
    return (2.0 * jnp.pi / length) * product_idx.astype(jnp.float32)


def tables(length, mode_count):
    cell_idx = jnp.arange(length, dtype=jnp.int32)
    low_modes = jnp.arange(mode_count, dtype=jnp.int32)
    both_modes = jnp.concatenate([low_modes, low_modes + (length - mode_count)])
    along_w = angles(cell_idx, low_modes, length)
    cos_w = jnp.cos(along_w)
    sin_w = jnp.sin(along_w)
    row_table = jnp.stack([cos_w, -sin_w], axis=1).astype(jnp.bfloat16)
    weight = jnp.where(low_modes == 0, 1.0, 2.0).astype(jnp.float32)[:, None]
    back_table = jnp.stack([weight * cos_w.T, -weight * sin_w.T], axis=1).astype(jnp.bfloat16)
    along_h = angles(cell_idx, both_modes, length)
    cos_h = jnp.cos(along_h)
    sin_h = jnp.sin(along_h)
    col_table = jnp.stack([jnp.stack([cos_h, -sin_h], axis=1), jnp.stack([sin_h, cos_h], axis=1)], axis=0).astype(jnp.bfloat16)
    return row_table, back_table, col_table


def product(form, left, right):
    return jnp.einsum(form, left.astype(jnp.float32), right.astype(jnp.float32), precision=lax.Precision.HIGHEST)


def mix_modes(spec_layer, mode_spec):
    real_weight = spec_layer[:, 0]
    imag_weight = spec_layer[:, 1]
    real_mode = mode_spec[:, :, 0]
    imag_mode = mode_spec[:, :, 1]
    out_real = product('koix,kix->kox', real_weight, real_mode) - product('koix,kix->kox', imag_weight, imag_mode)
    out_imag = product('koix,kix->kox', real_weight, imag_mode) + product('koix,kix->kox', imag_weight, real_mode)
    return jnp.stack([out_real, out_imag], axis=1)


def mix_adjoint(spec_layer, mode_spec, grad_mixed):
    real_weight = spec_layer[:, 0]
    imag_weight = spec_layer[:, 1]
    real_mode = mode_spec[:, :, 0]
    imag_mode = mode_spec[:, :, 1]
    real_grad = grad_mixed[:, 0]
    imag_grad = grad_mixed[:, 1]
    grad_real = product('koix,kox->kix', real_weight, real_grad) + product('koix,kox->kix', imag_weight, imag_grad)
    grad_imag = product('koix,kox->kix', real_weight, imag_grad) - product('koix,kox->kix', imag_weight, real_grad)
    spec_real = product('kox,kix->koix', real_grad, real_mode) + product('kox,kix->koix', imag_grad, imag_mode)
    spec_imag = product('kox,kix->koix', imag_grad, real_mode) - product('kox,kix->koix', real_grad, imag_mode)
    return jnp.stack([grad_real, grad_imag], axis=2), jnp.stack([spec_real, spec_imag], axis=1)


def layer_forward(activity, skip_layer, up_layer, down_layer, spec_layer, table_set):
    row_table, back_table, col_table = table_set
    length = activity.shape[2]
    row_spec = product('chw,wpk->kpch', activity, row_table).astype(jnp.bfloat16)
    mode_spec = (product('kpch,phqx->kcqx', row_spec, col_table) / length).astype(jnp.bfloat16)
    mixed_modes = mix_modes(spec_layer, mode_spec).astype(jnp.bfloat16)
    back_spec = product('kqcx,phqx->kpch', mixed_modes, col_table).astype(jnp.bfloat16)
    spectral = product('kpch,kpw->chw', back_spec, back_table) / length
    pre_act = spectral + product('oc,chw->ohw', skip_layer, activity)
    gated_act = smooth_gate(pre_act).astype(jnp.bfloat16)
    hidden = product('fc,chw->fhw', up_layer, gated_act)
    inner_act = smooth_gate(hidden).astype(jnp.bfloat16)
    result = (activity.astype(jnp.float32) + product('cf,fhw->chw', down_layer, inner_act)).astype(jnp.bfloat16)
    return result, (activity, mode_spec, pre_act, gated_act, hidden, inner_act)


def layer_backward(grad_out, saved_act, skip_layer, up_layer, down_layer, spec_layer, table_set):
    row_table, back_table, col_table = table_set
    activity, mode_spec, pre_act, gated_act, hidden, inner_act = saved_act
    length = activity.shape[2]
    grad_inner = product('cf,chw->fhw', down_layer, grad_out)
    grad_down = product('chw,fhw->cf', grad_out, inner_act) / length
    grad_hidden = (grad_inner * gate_slope(hidden)).astype(jnp.bfloat16)
    grad_gated = product('fc,fhw->chw', up_layer, grad_hidden)
    grad_up = product('fhw,chw->fc', grad_hidden, gated_act) / length
    grad_pre = (grad_gated * gate_slope(pre_act)).astype(jnp.bfloat16)
    grad_skip = product('ohw,chw->oc', grad_pre, activity) / length
    grad_back = (product('chw,kpw->kpch', grad_pre, back_table) / length).astype(jnp.bfloat16)
    grad_mixed = product('kpch,phqx->kqcx', grad_back, col_table).astype(jnp.bfloat16)
    grad_modes, grad_spec = mix_adjoint(spec_layer, mode_spec, grad_mixed)
    grad_rows = (product('kcqx,phqx->kpch', grad_modes.astype(jnp.bfloat16), col_table) / length).astype(jnp.bfloat16)
    grad_field = grad_out.astype(jnp.float32) + product('oc,ohw->chw', skip_layer, grad_pre) + product('kpch,wpk->chw', grad_rows, row_table)
    return grad_field.astype(jnp.bfloat16), grad_skip, grad_up, grad_down, grad_spec


def reference(emitted, returned, stash, skip_w, up_w, down_w, spec_w):
    length = emitted.shape[3]
    table_set = tables(length, M)
    ahead_all = jnp.roll(emitted, 1, axis=0)
    top_all = jnp.roll(returned, -1, axis=0)
    kept_all = jnp.roll(stash, SECTIONS // 2, axis=0)

    def section_work(inputs):
        ahead_input, top_grad, kept_input, skip_section, up_section, down_section, spec_section = inputs
        activity = ahead_input
        for layer_idx in range(LAYERS):
            activity, unused_keep = layer_forward(activity, skip_section[layer_idx], up_section[layer_idx], down_section[layer_idx], spec_section[layer_idx], table_set)
        sent_out = activity
        activity = kept_input
        saved_list = []
        for layer_idx in range(LAYERS):
            activity, layer_keep = layer_forward(activity, skip_section[layer_idx], up_section[layer_idx], down_section[layer_idx], spec_section[layer_idx], table_set)
            saved_list.append(layer_keep)
        grad_now = top_grad
        skip_list, up_list, down_list, spec_list = [], [], [], []
        for layer_idx in reversed(range(LAYERS)):
            grad_now, grad_skip, grad_up, grad_down, grad_spec = layer_backward(grad_now, saved_list[layer_idx], skip_section[layer_idx], up_section[layer_idx], down_section[layer_idx], spec_section[layer_idx], table_set)
            skip_list.insert(0, grad_skip)
            up_list.insert(0, grad_up)
            down_list.insert(0, grad_down)
            spec_list.insert(0, grad_spec)
        return sent_out, grad_now, jnp.stack(skip_list), jnp.stack(up_list), jnp.stack(down_list), jnp.stack(spec_list)

    sent, back_grad, grad_skip, grad_up, grad_down, grad_spec = lax.map(section_work, (ahead_all, top_all, kept_all, skip_w, up_w, down_w, spec_w))
    return (sent, back_grad, grad_skip, grad_up, grad_down, grad_spec)
```

```python
import jax
import jax.numpy as jnp
import numpy as np
from jax import lax
from jax.experimental import pallas as pl
from jax.experimental.pallas import tpu as pltpu
from jax.sharding import PartitionSpec as P

M = 64
LAYERS = 2


root_two_pi = 0.7978845608028654
cubic_coef = 0.044715


def from_partner(array, axis, stride):
    return lax.ppermute(array, axis, [(i, i ^ 1 << stride) for i in range(lax.axis_size(axis))])


def passed_along(block, axis, distance):
    devices = range(lax.axis_size(axis))
    route = [((i - distance) % len(devices), i) for i in devices]
    return lax.ppermute(block, axis, route)


def smooth_gate(values):
    return (
        0.5
        * values
        * (1.0 + jnp.tanh(root_two_pi * (values + cubic_coef * values * values * values)))
    )


def gate_slope(values):
    tangent = jnp.tanh(root_two_pi * (values + cubic_coef * values * values * values))
    return 0.5 * (1.0 + tangent) + 0.5 * values * (1.0 - tangent * tangent) * root_two_pi * (
        1.0 + 3.0 * cubic_coef * values * values
    )


def angles(left_idx, right_idx, length):
    product_idx = left_idx[:, None] * right_idx[None, :] % length
    return 2.0 * jnp.pi / length * product_idx.astype(jnp.float32)


def tables(length, mode_count):
    cell_idx = jnp.arange(length, dtype=jnp.int32)
    low_modes = jnp.arange(mode_count, dtype=jnp.int32)
    both_modes = jnp.concatenate([low_modes, low_modes + (length - mode_count)])
    along_w = angles(cell_idx, low_modes, length)
    cos_w = jnp.cos(along_w)
    sin_w = jnp.sin(along_w)
    row_table = jnp.stack([cos_w, -sin_w], axis=1).astype(jnp.bfloat16)
    weight = jnp.where(low_modes == 0, 1.0, 2.0).astype(jnp.float32)[:, None]
    back_table = jnp.stack([weight * cos_w.T, -weight * sin_w.T], axis=1).astype(jnp.bfloat16)
    along_h = angles(cell_idx, both_modes, length)
    cos_h = jnp.cos(along_h)
    sin_h = jnp.sin(along_h)
    col_table = jnp.stack(
        [jnp.stack([cos_h, -sin_h], axis=1), jnp.stack([sin_h, cos_h], axis=1)], axis=0
    ).astype(jnp.bfloat16)
    return (row_table, back_table, col_table)


def product(form, left, right):
    return jnp.einsum(form, left, right, preferred_element_type=jnp.float32)


def to_modes(row_spec):
    return lax.all_to_all(row_spec, "slab", split_axis=0, concat_axis=3, tiled=True)


def to_rows(back_spec):
    return lax.all_to_all(back_spec, "slab", split_axis=3, concat_axis=0, tiled=True)


def fetch_saved(saved_input):
    top_bit = lax.axis_size("section").bit_length() - 1
    return from_partner(saved_input, "section", top_bit - 1)


def mix_modes(spec_layer, mode_spec):
    real_weight = spec_layer[:, 0]
    imag_weight = spec_layer[:, 1]
    real_mode = mode_spec[:, :, 0]
    imag_mode = mode_spec[:, :, 1]
    out_real = product("koix,kix->kox", real_weight, real_mode) - product(
        "koix,kix->kox", imag_weight, imag_mode
    )
    out_imag = product("koix,kix->kox", real_weight, imag_mode) + product(
        "koix,kix->kox", imag_weight, real_mode
    )
    return jnp.stack([out_real, out_imag], axis=1)


def mix_adjoint(spec_layer, mode_spec, grad_mixed):
    real_weight = spec_layer[:, 0]
    imag_weight = spec_layer[:, 1]
    real_mode = mode_spec[:, :, 0]
    imag_mode = mode_spec[:, :, 1]
    real_grad = grad_mixed[:, 0]
    imag_grad = grad_mixed[:, 1]
    grad_real = product("koix,kox->kix", real_weight, real_grad) + product(
        "koix,kox->kix", imag_weight, imag_grad
    )
    grad_imag = product("koix,kox->kix", real_weight, imag_grad) - product(
        "koix,kox->kix", imag_weight, real_grad
    )
    spec_real = product("kox,kix->koix", real_grad, real_mode) + product(
        "kox,kix->koix", imag_grad, imag_mode
    )
    spec_imag = product("kox,kix->koix", imag_grad, real_mode) - product(
        "kox,kix->koix", real_grad, imag_mode
    )
    return (jnp.stack([grad_real, grad_imag], axis=2), jnp.stack([spec_real, spec_imag], axis=1))


def layer_forward(activity, skip_layer, up_layer, down_layer, spec_layer, table_set):
    row_table, back_table, col_table = table_set
    length = activity.shape[2]
    row_spec = to_modes(product("chw,wpk->kpch", activity, row_table).astype(jnp.bfloat16))
    mode_spec = (product("kpch,phqx->kcqx", row_spec, col_table) / length).astype(jnp.bfloat16)
    mixed_modes = mix_modes(spec_layer, mode_spec).astype(jnp.bfloat16)
    back_spec = to_rows(product("kqcx,phqx->kpch", mixed_modes, col_table).astype(jnp.bfloat16))
    spectral = product("kpch,kpw->chw", back_spec, back_table) / length
    pre_act = spectral + product("oc,chw->ohw", skip_layer, activity)
    gated_act = smooth_gate(pre_act).astype(jnp.bfloat16)
    hidden = product("fc,chw->fhw", up_layer, gated_act)
    inner_act = smooth_gate(hidden).astype(jnp.bfloat16)
    result = (activity.astype(jnp.float32) + product("cf,fhw->chw", down_layer, inner_act)).astype(
        jnp.bfloat16
    )
    return (result, (activity, mode_spec, pre_act, gated_act, hidden, inner_act))


def layer_backward(grad_out, saved_act, skip_layer, up_layer, down_layer, spec_layer, table_set):
    row_table, back_table, col_table = table_set
    activity, mode_spec, pre_act, gated_act, hidden, inner_act = saved_act
    length = activity.shape[2]
    grad_inner = product("cf,chw->fhw", down_layer, grad_out)
    grad_down = product("chw,fhw->cf", grad_out, inner_act) / length
    grad_hidden = (grad_inner * gate_slope(hidden)).astype(jnp.bfloat16)
    grad_gated = product("fc,fhw->chw", up_layer, grad_hidden)
    grad_up = product("fhw,chw->fc", grad_hidden, gated_act) / length
    grad_pre = (grad_gated * gate_slope(pre_act)).astype(jnp.bfloat16)
    grad_skip = product("ohw,chw->oc", grad_pre, activity) / length
    grad_back = to_modes(
        (product("chw,kpw->kpch", grad_pre, back_table) / length).astype(jnp.bfloat16)
    )
    grad_mixed = product("kpch,phqx->kqcx", grad_back, col_table).astype(jnp.bfloat16)
    grad_modes, grad_spec = mix_adjoint(spec_layer, mode_spec, grad_mixed)
    grad_rows = to_rows(
        (product("kcqx,phqx->kpch", grad_modes.astype(jnp.bfloat16), col_table) / length).astype(
            jnp.bfloat16
        )
    )
    grad_field = (
        grad_out.astype(jnp.float32)
        + product("oc,ohw->chw", skip_layer, grad_pre)
        + product("kpch,wpk->chw", grad_rows, row_table)
    )
    return (grad_field.astype(jnp.bfloat16), grad_skip, grad_up, grad_down, grad_spec)


def shards(emitted, returned, stash, skip_w, up_w, down_w, spec_w):
    length = emitted.shape[3]
    table_set = tables(length, M)
    skip_section = skip_w[0]
    up_section = up_w[0]
    down_section = down_w[0]
    spec_section = spec_w[0]
    ahead_input = passed_along(emitted[0], "section", 1)
    top_grad = passed_along(returned[0], "section", -1)
    kept_input = fetch_saved(stash[0])
    activity = ahead_input
    for layer_idx in range(LAYERS):
        activity, unused_keep = layer_forward(
            activity,
            skip_section[layer_idx],
            up_section[layer_idx],
            down_section[layer_idx],
            spec_section[layer_idx],
            table_set,
        )
    sent_out = activity
    activity = kept_input
    saved_list = []
    for layer_idx in range(LAYERS):
        activity, layer_keep = layer_forward(
            activity,
            skip_section[layer_idx],
            up_section[layer_idx],
            down_section[layer_idx],
            spec_section[layer_idx],
            table_set,
        )
        saved_list.append(layer_keep)
    grad_now = top_grad
    skip_list, up_list, down_list, spec_list = ([], [], [], [])
    for layer_idx in reversed(range(LAYERS)):
        grad_now, grad_skip, grad_up, grad_down, grad_spec = layer_backward(
            grad_now,
            saved_list[layer_idx],
            skip_section[layer_idx],
            up_section[layer_idx],
            down_section[layer_idx],
            spec_section[layer_idx],
            table_set,
        )
        skip_list.insert(0, grad_skip)
        up_list.insert(0, grad_up)
        down_list.insert(0, grad_down)
        spec_list.insert(0, grad_spec)
    summed = lax.psum((jnp.stack(skip_list), jnp.stack(up_list), jnp.stack(down_list)), "slab")
    return (
        sent_out[None],
        grad_now[None],
        summed[0][None],
        summed[1][None],
        summed[2][None],
        jnp.stack(spec_list)[None],
    )


BF = jnp.bfloat16
F32 = jnp.float32
VM = 60 * 1024 * 1024


def fast_tables(length, mode_count, groups):
    ang = lambda a, b: (np.float32(2.0 * np.pi / length) * ((a[:, None] * b[None, :]) % length).astype(np.float32))
    cells = np.arange(length)
    low = np.arange(mode_count)
    both = np.concatenate([low, low + (length - mode_count)])
    along = ang(low, cells)
    cos_w, sin_w = np.cos(along), np.sin(along)
    weight = np.where(low == 0, 1.0, 2.0).astype(np.float32)[:, None]

    def grouped(a, b):
        a = a.reshape(groups, 1, mode_count // groups, length)
        b = b.reshape(groups, 1, mode_count // groups, length)
        return np.concatenate([a, b], axis=1).reshape(2 * mode_count, length)

    row = grouped(cos_w, -sin_w)
    back = grouped(weight * cos_w, -weight * sin_w)
    along_h = ang(cells, both)
    cos_h, sin_h = np.cos(along_h), np.sin(along_h)
    col = np.stack([np.concatenate([cos_h, -sin_h], 1), np.concatenate([sin_h, cos_h], 1)], 0)
    modes = col.shape[2]
    col = col.reshape(2, groups, length // groups, modes).transpose(1, 0, 2, 3).reshape(2 * length, modes)
    made = lambda t: jnp.asarray(t.astype(BF))
    return made(row), made(row.T), made(back), made(back.T), made(col), made(col.T)


def call(body, grid, ins, outs, scratch, aliases=None, cost=(0, 0)):
    return pl.pallas_call(
        body,
        grid=grid,
        in_specs=ins,
        out_specs=outs[0],
        out_shape=outs[1],
        scratch_shapes=scratch,
        input_output_aliases=aliases or {},
        compiler_params=pltpu.CompilerParams(
            dimension_semantics=("arbitrary",) * len(grid), vmem_limit_bytes=VM
        ),
        cost_estimate=pl.CostEstimate(flops=cost[0], bytes_accessed=cost[1], transcendentals=0),
    )


def same(shape):
    return pl.BlockSpec(shape, lambda i: (0,) * len(shape))


def dot(a, b, ca=1, cb=0):
    return lax.dot_general(a, b, (((ca,), (cb,)), ((), ())), preferred_element_type=F32)


def first_rows(field, row):
    C, H, W = field.shape
    J = row.shape[0]
    cb = next(n for n in (5, 4, 2, 1) if C % n == 0)

    def body(v_ref, row_ref, out_ref):
        v = v_ref[...].reshape(cb * H, W)
        out_ref[...] = dot(row_ref[...], v, 1, 1).astype(BF)

    return call(
        body, (C // cb,),
        [pl.BlockSpec((cb, H, W), lambda i: (i, 0, 0)), same((J, W))],
        (pl.BlockSpec((J, cb * H), lambda i: (0, i)), jax.ShapeDtypeStruct((J, C * H), BF)),
        [], cost=(2 * J * C * H * W, 2 * C * H * W),
    )(field, row)


def gather_modes(src_ref, lhs, C, S, K, H):
    for c in range(C):
        for s in range(S):
            for p in range(2):
                j = s * 2 + p
                lhs[c * K:(c + 1) * K, j * H:(j + 1) * H] = src_ref[s, p * K:(p + 1) * K, c * H:(c + 1) * H]


def spread_modes(wide, out_ref, C, S, K, H):
    for c in range(C):
        for s in range(S):
            for p in range(2):
                j = s * 2 + p
                out_ref[s, p * K:(p + 1) * K, c * H:(c + 1) * H] = wide[c * K:(c + 1) * K, j * H:(j + 1) * H].astype(BF)


def split_parts(wide, parts):
    rows, X = parts.shape
    parts[:rows // 2, :] = wide[:, :X]
    parts[rows // 2:, :] = wide[:, X:]


def joined_parts(parts):
    rows = parts.shape[0] // 2
    return jnp.concatenate([parts[:rows, :], parts[rows:, :]], axis=1).astype(BF)


def modes_forward(spec, layer, src, col, col_t, length):
    _, K, _, C, _, X = spec.shape
    S, _, CH = src.shape
    H = CH // C

    def body(r_ref, src_ref, col_ref, colt_ref, out_ref, x_ref, lhs, xs, ys):
        k = pl.program_id(0)

        @pl.when(k == 0)
        def _():
            gather_modes(src_ref, lhs, C, S, K, H)
            x_ref[...] = (dot(lhs[...], col_ref[...]) / length).astype(BF)
            split_parts(x_ref[...].astype(F32), xs)

        real, imag = pl.ds(k, C, stride=K), pl.ds(C * K + k, C, stride=K)
        xr = xs[real, :][None]
        xi = xs[imag, :][None]
        rr = r_ref[0, 0, 0].astype(F32)
        ri = r_ref[0, 0, 1].astype(F32)
        ys[real, :] = jnp.sum(rr * xr - ri * xi, axis=1)
        ys[imag, :] = jnp.sum(rr * xi + ri * xr, axis=1)

        @pl.when(k == K - 1)
        def _():
            spread_modes(dot(joined_parts(ys), colt_ref[...]), out_ref, C, S, K, H)

    J = col.shape[0]
    return call(
        body, (K,),
        [pl.BlockSpec((1, 1, 2, C, C, X), lambda i: (layer, i, 0, 0, 0, 0)), same(src.shape), same(col.shape), same(col_t.shape)],
        ([same(src.shape), same((C * K, 2 * X))],
         [jax.ShapeDtypeStruct(src.shape, BF), jax.ShapeDtypeStruct((C * K, 2 * X), BF)]),
        [pltpu.VMEM((C * K, J), BF), pltpu.VMEM((2 * C * K, X), F32), pltpu.VMEM((2 * C * K, X), F32)],
        cost=(8 * C * K * J * X, 8 * K * C * C * X),
    )(spec, src, col, col_t)


def modes_backward(spec, layer, src, kept_modes, col, col_t, length, held):
    L, K, _, C, _, X = spec.shape
    S, _, CH = src.shape
    H = CH // C

    def body(r_ref, src_ref, m_ref, col_ref, colt_ref, *rest):
        out_ref, grad_ref, lhs, xs, gs, ys = rest[-6:]
        k = pl.program_id(0)

        @pl.when(k == 0)
        def _():
            gather_modes(src_ref, lhs, C, S, K, H)
            split_parts(dot(lhs[...], col_ref[...]).astype(BF).astype(F32), gs)
            split_parts(m_ref[...].astype(F32), xs)

        real, imag = pl.ds(k, C, stride=K), pl.ds(C * K + k, C, stride=K)
        xr = xs[real, :][None]
        xi = xs[imag, :][None]
        gr = gs[real, :][:, None, :]
        gi = gs[imag, :][:, None, :]
        rr = r_ref[0, 0, 0].astype(F32)
        ri = r_ref[0, 0, 1].astype(F32)
        ys[real, :] = jnp.sum(rr * gr + ri * gi, axis=0)
        ys[imag, :] = jnp.sum(rr * gi - ri * gr, axis=0)
        grad_ref[0, 0, 0] = gr * xr + gi * xi
        grad_ref[0, 0, 1] = gi * xr - gr * xi

        @pl.when(k == K - 1)
        def _():
            spread_modes(dot(joined_parts(ys), colt_ref[...]) / length, out_ref, C, S, K, H)

    J = col.shape[0]
    block = pl.BlockSpec((1, 1, 2, C, C, X), lambda i: (layer, i, 0, 0, 0, 0))
    ins = [block, same(src.shape), same(kept_modes.shape), same(col.shape), same(col_t.shape)]
    args = [spec, src, kept_modes, col, col_t]
    aliases = {}
    if held is not None:
        ins.append(pl.BlockSpec(memory_space=pl.ANY))
        args.append(held)
        aliases = {5: 1}
    return call(
        body, (K,), ins,
        ([same(src.shape), block], [jax.ShapeDtypeStruct(src.shape, BF), jax.ShapeDtypeStruct(spec.shape, F32)]),
        [pltpu.VMEM((C * K, J), BF)] + [pltpu.VMEM((2 * C * K, X), F32)] * 3,
        aliases, cost=(8 * C * K * J * X, 16 * K * C * C * X),
    )(*args)


def load_rows(src_ref, turned, C, CP, H):
    J = turned.shape[1]
    turned[...] = jnp.zeros_like(turned)
    for c in range(C):
        tile = src_ref[:, c * H:(c + 1) * H].astype(F32)
        turned[pl.ds(c, H, stride=CP), :] = tile.T


def store_rows(turned, out_ref, C, CP, H):
    for c in range(C):
        tile = turned[pl.ds(c, H, stride=CP), :]
        out_ref[:, c * H:(c + 1) * H] = tile.T.astype(BF)


def tanh_of(t, t2):
    return jnp.tanh(t * (root_two_pi + (root_two_pi * cubic_coef) * t2))


def gate(t):
    half = 0.5 * t
    return half + half * tanh_of(t, t * t)


def gate_pair(t):
    t2 = t * t
    th = tanh_of(t, t2)
    near = 0.5 + 0.5 * th
    half = 0.5 * t
    slope = near + half * (1.0 - th * th) * (root_two_pi + (3.0 * cubic_coef * root_two_pi) * t2)
    return t * near, slope


HB = 16


def field_forward(v, src, skip, up, down, back, row_t, length, want_rows):
    H, CP, W = v.shape
    J = back.shape[0]
    C = src.shape[1] // H
    F = up.shape[0]
    steps = H // HB

    def body(v_ref, src_ref, skip_ref, up_ref, down_ref, back_ref, rowt_ref, *rest):
        if want_rows:
            out_ref, rows_ref, turned, zs, made = rest
        else:
            out_ref, turned, zs = rest
        i = pl.program_id(0)

        @pl.when(i == 0)
        def _():
            load_rows(src_ref, turned, C, CP, H)

        at = pl.ds(pl.multiple_of(i * HB * CP, HB * CP), HB * CP)
        zs[...] = dot(turned[at, :].astype(BF), back_ref[...]) / length

        def one(h, carry):
            vh = v_ref[h]
            z = zs[pl.ds(pl.multiple_of(h * CP, CP), CP), :] + dot(skip_ref[...], vh)
            y = gate(z).astype(BF)
            act = gate(dot(up_ref[...], y)).astype(BF)
            out_ref[h] = (vh.astype(F32) + dot(down_ref[...], act)).astype(BF)
            return carry

        lax.fori_loop(0, HB, one, 0, unroll=4)
        if want_rows:
            made[at, :] = dot(out_ref[...].reshape(HB * CP, W), rowt_ref[...])

            @pl.when(i == steps - 1)
            def _():
                store_rows(made, rows_ref, C, CP, H)

    block = pl.BlockSpec((HB, CP, W), lambda i: (i, 0, 0))
    outs = ([block], [jax.ShapeDtypeStruct(v.shape, BF)])
    scratch = [pltpu.VMEM((H * CP, J), F32), pltpu.VMEM((HB * CP, W), F32)]
    if want_rows:
        outs[0].append(same((J, C * H)))
        outs[1].append(jax.ShapeDtypeStruct((J, C * H), BF))
        scratch.append(pltpu.VMEM((H * CP, J), F32))
    return call(
        body, (steps,),
        [block, same(src.shape), same(skip.shape), same(up.shape), same(down.shape), same(back.shape), same(row_t.shape)],
        outs, scratch, cost=(4 * H * CP * W * (F + J), 4 * H * CP * W),
    )(v, src, skip, up, down, back, row_t)


def field_backward(v, g, src, skip, up, down, up_t, down_t, back, back_t, length):
    H, CP, W = v.shape
    J = back.shape[0]
    C = src.shape[1] // H
    F = up.shape[0]
    steps = H // HB

    def body(v_ref, g_ref, src_ref, skip_ref, up_ref, down_ref, upt_ref, downt_ref, back_ref, backt_ref,
             gz_ref, rows_ref, gskip_ref, gup_ref, gdown_ref, turned, zs, made):
        i = pl.program_id(0)

        @pl.when(i == 0)
        def _():
            load_rows(src_ref, turned, C, CP, H)
            gskip_ref[...] = jnp.zeros_like(gskip_ref)
            gup_ref[...] = jnp.zeros_like(gup_ref)
            gdown_ref[...] = jnp.zeros_like(gdown_ref)

        at = pl.ds(pl.multiple_of(i * HB * CP, HB * CP), HB * CP)
        zs[...] = dot(turned[at, :].astype(BF), back_ref[...]) / length

        def one(h, carry):
            vh = v_ref[h]
            gh = g_ref[h]
            z = zs[pl.ds(pl.multiple_of(h * CP, CP), CP), :] + dot(skip_ref[...], vh)
            y, y_slope = gate_pair(z)
            y = y.astype(BF)
            act, act_slope = gate_pair(dot(up_ref[...], y))
            act = act.astype(BF)
            grad_hidden = (dot(downt_ref[...], gh) * act_slope).astype(BF)
            gz = (dot(upt_ref[...], grad_hidden) * y_slope).astype(BF)
            gz_ref[h] = gz
            gdown_ref[...] += dot(gh, act, 1, 1)
            gup_ref[...] += dot(grad_hidden, y, 1, 1)
            gskip_ref[...] += dot(gz, vh, 1, 1)
            return carry

        lax.fori_loop(0, HB, one, 0, unroll=2)
        made[at, :] = dot(gz_ref[...].reshape(HB * CP, W), backt_ref[...]) / length

        @pl.when(i == steps - 1)
        def _():
            store_rows(made, rows_ref, C, CP, H)

    block = pl.BlockSpec((HB, CP, W), lambda i: (i, 0, 0))
    args = (v, g, src, skip, up, down, up_t, down_t, back, back_t)
    small = [(CP, CP), (F, CP), (CP, F)]
    return call(
        body, (steps,),
        [block, block] + [same(a.shape) for a in args[2:]],
        ([block, same((J, C * H))] + [same(s) for s in small],
         [jax.ShapeDtypeStruct(v.shape, BF), jax.ShapeDtypeStruct((J, C * H), BF)]
         + [jax.ShapeDtypeStruct(s, F32) for s in small]),
        [pltpu.VMEM((H * CP, J), F32), pltpu.VMEM((HB * CP, W), F32), pltpu.VMEM((H * CP, J), F32)],
        cost=(8 * H * CP * W * (F + J), 6 * H * CP * W),
    )(*args)


def field_grad(g, gz, src, skip_t, row):
    H, CP, W = g.shape
    J = row.shape[0]
    C = src.shape[1] // H
    steps = H // HB

    def body(g_ref, gz_ref, src_ref, skipt_ref, row_ref, out_ref, turned, zs):
        i = pl.program_id(0)

        @pl.when(i == 0)
        def _():
            load_rows(src_ref, turned, C, CP, H)

        at = pl.ds(pl.multiple_of(i * HB * CP, HB * CP), HB * CP)
        zs[...] = dot(turned[at, :].astype(BF), row_ref[...])

        def one(h, carry):
            here = pl.ds(pl.multiple_of(h * CP, CP), CP)
            out_ref[h] = (g_ref[h].astype(F32) + dot(skipt_ref[...], gz_ref[h]) + zs[here, :]).astype(BF)
            return carry

        lax.fori_loop(0, HB, one, 0, unroll=4)

    block = pl.BlockSpec((HB, CP, W), lambda i: (i, 0, 0))
    return call(
        body, (steps,),
        [block, block, same(src.shape), same(skip_t.shape), same(row.shape)],
        (block, jax.ShapeDtypeStruct(g.shape, BF)),
        [pltpu.VMEM((H * CP, J), F32), pltpu.VMEM((HB * CP, W), F32)],
        cost=(2 * H * CP * W * J, 6 * H * CP * W),
    )(g, gz, src, skip_t, row)


def exchanged(spectra, groups):
    blocks = spectra.reshape(groups, spectra.size // spectra.shape[-1] // groups, spectra.shape[-1])
    return lax.all_to_all(blocks, "slab", split_axis=0, concat_axis=0, tiled=True)


def fast_shards(emitted, returned, stash, skip_w, up_w, down_w, spec_w):
    _, C, H, W = emitted.shape
    L = spec_w.shape[1]
    S = lax.axis_size("slab")
    mode_count = spec_w.shape[2] * S
    CP = -(-C // 16) * 16
    row, row_t, back, back_t, col, col_t = fast_tables(W, mode_count, S)
    spec = spec_w[0]
    pad = CP - C
    skip = jnp.pad(skip_w[0], ((0, 0), (0, pad), (0, pad)))
    up = jnp.pad(up_w[0], ((0, 0), (0, 0), (0, pad)))
    down = jnp.pad(down_w[0], ((0, 0), (0, pad), (0, 0)))
    turn = lambda a: jnp.swapaxes(a, 1, 2)
    skip_t, up_t, down_t = turn(skip), turn(up), turn(down)
    size = lax.axis_size("section")
    lined = lambda f: jnp.pad(jnp.swapaxes(f, 0, 1), ((0, 0), (0, pad), (0, 0)))
    plain = lambda f: jnp.swapaxes(f[:, :C], 0, 1)
    flat = lambda a: a.reshape(-1, a.shape[-1])

    ahead = passed_along(emitted[0], "section", 1)
    rows_a = passed_along(exchanged(first_rows(emitted[0], row), S), "section", 1)
    rows_k = passed_along(exchanged(first_rows(stash[0], row), S), "section", size // 2)
    kept = passed_along(stash[0], "section", size // 2)
    top = passed_along(returned[0], "section", -1)

    ahead = lined(ahead)
    for l in range(L):
        mixed, _ = modes_forward(spec, l, rows_a, col, col_t, W)
        made = field_forward(ahead, flat(exchanged(mixed, S)), skip[l], up[l], down[l], back, row_t, W, l < L - 1)
        ahead = made[0]
        if l < L - 1:
            rows_a = exchanged(made[1], S)
    sent = plain(ahead)

    kept = lined(kept)
    saved = []
    for l in range(L):
        mixed, modes = modes_forward(spec, l, rows_k, col, col_t, W)
        arrived = flat(exchanged(mixed, S))
        saved.append((kept, arrived, modes))
        if l < L - 1:
            kept, rows_k = field_forward(kept, arrived, skip[l], up[l], down[l], back, row_t, W, True)
            rows_k = exchanged(rows_k, S)
    g = lined(top)
    spec_grad = None
    skips, ups, downs = [], [], []
    for l in reversed(range(L)):
        v, arrived, modes = saved[l]
        gz, rows, gs, gu, gd = field_backward(v, g, arrived, skip[l], up[l], down[l], up_t[l], down_t[l], back, back_t, W)
        mixed, spec_grad = modes_backward(spec, l, exchanged(rows, S), modes, col, col_t, W, spec_grad)
        g = field_grad(g, gz, flat(exchanged(mixed, S)), skip_t[l], row)
        skips.insert(0, gs[:C, :C])
        ups.insert(0, gu[:, :C])
        downs.insert(0, gd[:C])
    summed = lax.psum((jnp.stack(skips) / W, jnp.stack(ups) / W, jnp.stack(downs) / W), "slab")
    return (sent[None], plain(g)[None], summed[0][None], summed[1][None], summed[2][None], spec_grad[None])


def work(*args):
    H = args[0].shape[2]
    K = args[6].shape[2]
    if H % 128 == 0 and K % 16 == 0 and H % HB == 0 and args[6].shape[6] == 128 and 2 * K * lax.axis_size("slab") == 128:
        return fast_shards(*args)
    return shards(*args)


def solution(mesh):
    placed = (
        P("section", None, "slab", None),
        P("section", None, "slab", None),
        P("section", None, "slab", None),
        P("section", None, None, None),
        P("section", None, None, None),
        P("section", None, None, None),
        P("section", None, "slab", None, None, None, None),
    )
    return jax.shard_map(
        work,
        mesh=mesh,
        in_specs=placed,
        out_specs=(
            P("section", None, "slab", None),
            P("section", None, "slab", None),
            P("section", None, None, None),
            P("section", None, None, None),
            P("section", None, None, None),
            P("section", None, "slab", None, None, None, None),
        ),
        check_vma=False,
    )
```

```python
import jax
import jax.numpy as jnp
import numpy as np
from jax import lax
from jax.experimental import pallas as pl
from jax.experimental.pallas import tpu as pltpu
from jax.sharding import PartitionSpec as P

M = 64
LAYERS = 2


root_two_pi = 0.7978845608028654
cubic_coef = 0.044715


def from_partner(array, axis, stride):
    return lax.ppermute(array, axis, [(i, i ^ 1 << stride) for i in range(lax.axis_size(axis))])


def passed_along(block, axis, distance):
    devices = range(lax.axis_size(axis))
    route = [((i - distance) % len(devices), i) for i in devices]
    return lax.ppermute(block, axis, route)


def smooth_gate(values):
    return (
        0.5
        * values
        * (1.0 + jnp.tanh(root_two_pi * (values + cubic_coef * values * values * values)))
    )


def gate_slope(values):
    tangent = jnp.tanh(root_two_pi * (values + cubic_coef * values * values * values))
    return 0.5 * (1.0 + tangent) + 0.5 * values * (1.0 - tangent * tangent) * root_two_pi * (
        1.0 + 3.0 * cubic_coef * values * values
    )


def angles(left_idx, right_idx, length):
    product_idx = left_idx[:, None] * right_idx[None, :] % length
    return 2.0 * jnp.pi / length * product_idx.astype(jnp.float32)


def tables(length, mode_count):
    cell_idx = jnp.arange(length, dtype=jnp.int32)
    low_modes = jnp.arange(mode_count, dtype=jnp.int32)
    both_modes = jnp.concatenate([low_modes, low_modes + (length - mode_count)])
    along_w = angles(cell_idx, low_modes, length)
    cos_w = jnp.cos(along_w)
    sin_w = jnp.sin(along_w)
    row_table = jnp.stack([cos_w, -sin_w], axis=1).astype(jnp.bfloat16)
    weight = jnp.where(low_modes == 0, 1.0, 2.0).astype(jnp.float32)[:, None]
    back_table = jnp.stack([weight * cos_w.T, -weight * sin_w.T], axis=1).astype(jnp.bfloat16)
    along_h = angles(cell_idx, both_modes, length)
    cos_h = jnp.cos(along_h)
    sin_h = jnp.sin(along_h)
    col_table = jnp.stack(
        [jnp.stack([cos_h, -sin_h], axis=1), jnp.stack([sin_h, cos_h], axis=1)], axis=0
    ).astype(jnp.bfloat16)
    return (row_table, back_table, col_table)


def product(form, left, right):
    return jnp.einsum(form, left, right, preferred_element_type=jnp.float32)


def to_modes(row_spec):
    return lax.all_to_all(row_spec, "slab", split_axis=0, concat_axis=3, tiled=True)


def to_rows(back_spec):
    return lax.all_to_all(back_spec, "slab", split_axis=3, concat_axis=0, tiled=True)


def fetch_saved(saved_input):
    top_bit = lax.axis_size("section").bit_length() - 1
    return from_partner(saved_input, "section", top_bit - 1)


def mix_modes(spec_layer, mode_spec):
    real_weight = spec_layer[:, 0]
    imag_weight = spec_layer[:, 1]
    real_mode = mode_spec[:, :, 0]
    imag_mode = mode_spec[:, :, 1]
    out_real = product("koix,kix->kox", real_weight, real_mode) - product(
        "koix,kix->kox", imag_weight, imag_mode
    )
    out_imag = product("koix,kix->kox", real_weight, imag_mode) + product(
        "koix,kix->kox", imag_weight, real_mode
    )
    return jnp.stack([out_real, out_imag], axis=1)


def mix_adjoint(spec_layer, mode_spec, grad_mixed):
    real_weight = spec_layer[:, 0]
    imag_weight = spec_layer[:, 1]
    real_mode = mode_spec[:, :, 0]
    imag_mode = mode_spec[:, :, 1]
    real_grad = grad_mixed[:, 0]
    imag_grad = grad_mixed[:, 1]
    grad_real = product("koix,kox->kix", real_weight, real_grad) + product(
        "koix,kox->kix", imag_weight, imag_grad
    )
    grad_imag = product("koix,kox->kix", real_weight, imag_grad) - product(
        "koix,kox->kix", imag_weight, real_grad
    )
    spec_real = product("kox,kix->koix", real_grad, real_mode) + product(
        "kox,kix->koix", imag_grad, imag_mode
    )
    spec_imag = product("kox,kix->koix", imag_grad, real_mode) - product(
        "kox,kix->koix", real_grad, imag_mode
    )
    return (jnp.stack([grad_real, grad_imag], axis=2), jnp.stack([spec_real, spec_imag], axis=1))


def layer_forward(activity, skip_layer, up_layer, down_layer, spec_layer, table_set):
    row_table, back_table, col_table = table_set
    length = activity.shape[2]
    row_spec = to_modes(product("chw,wpk->kpch", activity, row_table).astype(jnp.bfloat16))
    mode_spec = (product("kpch,phqx->kcqx", row_spec, col_table) / length).astype(jnp.bfloat16)
    mixed_modes = mix_modes(spec_layer, mode_spec).astype(jnp.bfloat16)
    back_spec = to_rows(product("kqcx,phqx->kpch", mixed_modes, col_table).astype(jnp.bfloat16))
    spectral = product("kpch,kpw->chw", back_spec, back_table) / length
    pre_act = spectral + product("oc,chw->ohw", skip_layer, activity)
    gated_act = smooth_gate(pre_act).astype(jnp.bfloat16)
    hidden = product("fc,chw->fhw", up_layer, gated_act)
    inner_act = smooth_gate(hidden).astype(jnp.bfloat16)
    result = (activity.astype(jnp.float32) + product("cf,fhw->chw", down_layer, inner_act)).astype(
        jnp.bfloat16
    )
    return (result, (activity, mode_spec, pre_act, gated_act, hidden, inner_act))


def layer_backward(grad_out, saved_act, skip_layer, up_layer, down_layer, spec_layer, table_set):
    row_table, back_table, col_table = table_set
    activity, mode_spec, pre_act, gated_act, hidden, inner_act = saved_act
    length = activity.shape[2]
    grad_inner = product("cf,chw->fhw", down_layer, grad_out)
    grad_down = product("chw,fhw->cf", grad_out, inner_act) / length
    grad_hidden = (grad_inner * gate_slope(hidden)).astype(jnp.bfloat16)
    grad_gated = product("fc,fhw->chw", up_layer, grad_hidden)
    grad_up = product("fhw,chw->fc", grad_hidden, gated_act) / length
    grad_pre = (grad_gated * gate_slope(pre_act)).astype(jnp.bfloat16)
    grad_skip = product("ohw,chw->oc", grad_pre, activity) / length
    grad_back = to_modes(
        (product("chw,kpw->kpch", grad_pre, back_table) / length).astype(jnp.bfloat16)
    )
    grad_mixed = product("kpch,phqx->kqcx", grad_back, col_table).astype(jnp.bfloat16)
    grad_modes, grad_spec = mix_adjoint(spec_layer, mode_spec, grad_mixed)
    grad_rows = to_rows(
        (product("kcqx,phqx->kpch", grad_modes.astype(jnp.bfloat16), col_table) / length).astype(
            jnp.bfloat16
        )
    )
    grad_field = (
        grad_out.astype(jnp.float32)
        + product("oc,ohw->chw", skip_layer, grad_pre)
        + product("kpch,wpk->chw", grad_rows, row_table)
    )
    return (grad_field.astype(jnp.bfloat16), grad_skip, grad_up, grad_down, grad_spec)


def shards(emitted, returned, stash, skip_w, up_w, down_w, spec_w):
    length = emitted.shape[3]
    table_set = tables(length, M)
    skip_section = skip_w[0]
    up_section = up_w[0]
    down_section = down_w[0]
    spec_section = spec_w[0]
    ahead_input = passed_along(emitted[0], "section", 1)
    top_grad = passed_along(returned[0], "section", -1)
    kept_input = fetch_saved(stash[0])
    activity = ahead_input
    for layer_idx in range(LAYERS):
        activity, unused_keep = layer_forward(
            activity,
            skip_section[layer_idx],
            up_section[layer_idx],
            down_section[layer_idx],
            spec_section[layer_idx],
            table_set,
        )
    sent_out = activity
    activity = kept_input
    saved_list = []
    for layer_idx in range(LAYERS):
        activity, layer_keep = layer_forward(
            activity,
            skip_section[layer_idx],
            up_section[layer_idx],
            down_section[layer_idx],
            spec_section[layer_idx],
            table_set,
        )
        saved_list.append(layer_keep)
    grad_now = top_grad
    skip_list, up_list, down_list, spec_list = ([], [], [], [])
    for layer_idx in reversed(range(LAYERS)):
        grad_now, grad_skip, grad_up, grad_down, grad_spec = layer_backward(
            grad_now,
            saved_list[layer_idx],
            skip_section[layer_idx],
            up_section[layer_idx],
            down_section[layer_idx],
            spec_section[layer_idx],
            table_set,
        )
        skip_list.insert(0, grad_skip)
        up_list.insert(0, grad_up)
        down_list.insert(0, grad_down)
        spec_list.insert(0, grad_spec)
    summed = lax.psum((jnp.stack(skip_list), jnp.stack(up_list), jnp.stack(down_list)), "slab")
    return (
        sent_out[None],
        grad_now[None],
        summed[0][None],
        summed[1][None],
        summed[2][None],
        jnp.stack(spec_list)[None],
    )


BF = jnp.bfloat16
F32 = jnp.float32
VM = 60 * 1024 * 1024


def fast_tables(length, mode_count, groups):
    ang = lambda a, b: (np.float32(2.0 * np.pi / length) * ((a[:, None] * b[None, :]) % length).astype(np.float32))
    cells = np.arange(length)
    low = np.arange(mode_count)
    both = np.concatenate([low, low + (length - mode_count)])
    along = ang(low, cells)
    cos_w, sin_w = np.cos(along), np.sin(along)
    weight = np.where(low == 0, 1.0, 2.0).astype(np.float32)[:, None]

    def grouped(a, b):
        a = a.reshape(groups, 1, mode_count // groups, length)
        b = b.reshape(groups, 1, mode_count // groups, length)
        return np.concatenate([a, b], axis=1).reshape(2 * mode_count, length)

    row = grouped(cos_w, -sin_w)
    back = grouped(weight * cos_w, -weight * sin_w)
    along_h = ang(cells, both)
    cos_h, sin_h = np.cos(along_h), np.sin(along_h)
    col = np.stack([np.concatenate([cos_h, -sin_h], 1), np.concatenate([sin_h, cos_h], 1)], 0)
    modes = col.shape[2]
    col = col.reshape(2, groups, length // groups, modes).transpose(1, 0, 2, 3).reshape(2 * length, modes)
    made = lambda t: jnp.asarray(t.astype(BF))
    return made(row), made(row.T), made(back), made(back.T), made(col), made(col.T)


def call(body, grid, ins, outs, scratch, aliases=None, cost=(0, 0)):
    return pl.pallas_call(
        body,
        grid=grid,
        in_specs=ins,
        out_specs=outs[0],
        out_shape=outs[1],
        scratch_shapes=scratch,
        input_output_aliases=aliases or {},
        compiler_params=pltpu.CompilerParams(
            dimension_semantics=("arbitrary",) * len(grid), vmem_limit_bytes=VM
        ),
        cost_estimate=pl.CostEstimate(flops=cost[0], bytes_accessed=cost[1], transcendentals=0),
    )


def same(shape):
    return pl.BlockSpec(shape, lambda i: (0,) * len(shape))


def dot(a, b, ca=1, cb=0):
    return lax.dot_general(a, b, (((ca,), (cb,)), ((), ())), preferred_element_type=F32)


def first_rows(field, row):
    C, H, W = field.shape
    J = row.shape[0]
    cb = next(n for n in (5, 4, 2, 1) if C % n == 0)

    def body(v_ref, row_ref, out_ref):
        v = v_ref[...].reshape(cb * H, W)
        out_ref[...] = dot(row_ref[...], v, 1, 1).astype(BF)

    return call(
        body, (C // cb,),
        [pl.BlockSpec((cb, H, W), lambda i: (i, 0, 0)), same((J, W))],
        (pl.BlockSpec((J, cb * H), lambda i: (0, i)), jax.ShapeDtypeStruct((J, C * H), BF)),
        [], cost=(2 * J * C * H * W, 2 * C * H * W),
    )(field, row)


def gather_modes(src_ref, lhs, C, S, K, H):
    for c in range(C):
        for s in range(S):
            for p in range(2):
                j = s * 2 + p
                lhs[c * K:(c + 1) * K, j * H:(j + 1) * H] = src_ref[s, p * K:(p + 1) * K, c * H:(c + 1) * H]


def spread_modes(wide, out_ref, C, S, K, H):
    for c in range(C):
        for s in range(S):
            for p in range(2):
                j = s * 2 + p
                out_ref[s, p * K:(p + 1) * K, c * H:(c + 1) * H] = wide[c * K:(c + 1) * K, j * H:(j + 1) * H].astype(BF)


def split_parts(wide, parts):
    rows, X = parts.shape
    parts[:rows // 2, :] = wide[:, :X]
    parts[rows // 2:, :] = wide[:, X:]


def joined_parts(parts):
    rows = parts.shape[0] // 2
    return jnp.concatenate([parts[:rows, :], parts[rows:, :]], axis=1).astype(BF)


def weave(pair, real, imag, C):
    even, odd = pl.ds(0, C, stride=2), pl.ds(1, C, stride=2)
    pair[0, even, :] = real
    pair[0, odd, :] = -imag
    pair[1, even, :] = imag
    pair[1, odd, :] = real


def modes_forward(spec, layer, src, col, col_t, length):
    _, K, C, _, X = spec.shape
    S, _, CH = src.shape
    H = CH // C

    def body(r_ref, src_ref, col_ref, colt_ref, out_ref, x_ref, lhs, xs, ys, pair):
        k = pl.program_id(0)

        @pl.when(k == 0)
        def _():
            gather_modes(src_ref, lhs, C, S, K, H)
            x_ref[...] = (dot(lhs[...], col_ref[...]) * (1.0 / length)).astype(BF)
            split_parts(x_ref[...].astype(F32), xs)

        real, imag = pl.ds(k, C, stride=K), pl.ds(C * K + k, C, stride=K)
        weave(pair, xs[real, :], xs[imag, :], C)
        held = r_ref[0, 0].astype(F32)
        ys[real, :] = jnp.sum(held * pair[0][None], axis=1)
        ys[imag, :] = jnp.sum(held * pair[1][None], axis=1)

        @pl.when(k == K - 1)
        def _():
            spread_modes(dot(joined_parts(ys), colt_ref[...]), out_ref, C, S, K, H)

    J = col.shape[0]
    return call(
        body, (K,),
        [pl.BlockSpec((1, 1, C, 2 * C, X), lambda i: (layer, i, 0, 0, 0)), same(src.shape), same(col.shape), same(col_t.shape)],
        ([same(src.shape), same((C * K, 2 * X))],
         [jax.ShapeDtypeStruct(src.shape, BF), jax.ShapeDtypeStruct((C * K, 2 * X), BF)]),
        [pltpu.VMEM((C * K, J), BF), pltpu.VMEM((2 * C * K, X), F32), pltpu.VMEM((2 * C * K, X), F32), pltpu.VMEM((2, 2 * C, X), F32)],
        cost=(8 * C * K * J * X, 8 * K * C * C * X),
    )(spec, src, col, col_t)


def modes_backward(spec, layer, src, kept_modes, col, col_t, length, held):
    L, K, C, _, X = spec.shape
    S, _, CH = src.shape
    H = CH // C

    def body(r_ref, src_ref, m_ref, col_ref, colt_ref, *rest):
        out_ref, grad_ref, lhs, xs, gs, ys, pair = rest[-7:]
        k = pl.program_id(0)

        @pl.when(k == 0)
        def _():
            gather_modes(src_ref, lhs, C, S, K, H)
            split_parts(dot(lhs[...], col_ref[...]).astype(BF).astype(F32), gs)
            split_parts(m_ref[...].astype(F32), xs)

        real, imag = pl.ds(k, C, stride=K), pl.ds(C * K + k, C, stride=K)
        gr = gs[real, :][:, None, :]
        gi = gs[imag, :][:, None, :]
        weave(pair, xs[real, :], xs[imag, :], C)
        grad_ref[0, 0] = gr * pair[0][None] + gi * pair[1][None]
        held = r_ref[0, 0].astype(F32)
        pair[0] = jnp.sum(held * gr, axis=0)
        pair[1] = jnp.sum(held * gi, axis=0)
        even, odd = pl.ds(0, C, stride=2), pl.ds(1, C, stride=2)
        ys[real, :] = pair[0, even, :] + pair[1, odd, :]
        ys[imag, :] = pair[1, even, :] - pair[0, odd, :]

        @pl.when(k == K - 1)
        def _():
            spread_modes(dot(joined_parts(ys), colt_ref[...]) * (1.0 / length), out_ref, C, S, K, H)

    J = col.shape[0]
    block = pl.BlockSpec((1, 1, C, 2 * C, X), lambda i: (layer, i, 0, 0, 0))
    ins = [block, same(src.shape), same(kept_modes.shape), same(col.shape), same(col_t.shape)]
    args = [spec, src, kept_modes, col, col_t]
    aliases = {}
    if held is not None:
        ins.append(pl.BlockSpec(memory_space=pl.ANY))
        args.append(held)
        aliases = {5: 1}
    return call(
        body, (K,), ins,
        ([same(src.shape), block], [jax.ShapeDtypeStruct(src.shape, BF), jax.ShapeDtypeStruct(spec.shape, F32)]),
        [pltpu.VMEM((C * K, J), BF)] + [pltpu.VMEM((2 * C * K, X), F32)] * 3 + [pltpu.VMEM((2, 2 * C, X), F32)],
        aliases, cost=(8 * C * K * J * X, 16 * K * C * C * X),
    )(*args)


def load_rows(src_ref, turned, C, CP, H):
    J = turned.shape[1]
    turned[...] = jnp.zeros_like(turned)
    for c in range(C):
        tile = src_ref[:, c * H:(c + 1) * H].astype(F32)
        turned[pl.ds(c, H, stride=CP), :] = tile.T


def store_rows(turned, out_ref, C, CP, H):
    for c in range(C):
        tile = turned[pl.ds(c, H, stride=CP), :]
        out_ref[:, c * H:(c + 1) * H] = tile.T.astype(BF)


def tanh_of(t, t2):
    return jnp.tanh(t * (root_two_pi + (root_two_pi * cubic_coef) * t2))


def gate(t):
    half = 0.5 * t
    return half + half * tanh_of(t, t * t)


def gate_pair(t):
    t2 = t * t
    th = tanh_of(t, t2)
    near = 0.5 + 0.5 * th
    half = 0.5 * t
    slope = near + half * (1.0 - th * th) * (root_two_pi + (3.0 * cubic_coef * root_two_pi) * t2)
    return t * near, slope


HB = 16
G = 8


def field_forward(v, src, skip, up, down, back, row_t, length, want_rows):
    H, CP, W = v.shape
    J = back.shape[0]
    C = src.shape[1] // H
    F = up.shape[0] // G
    steps = H // HB

    def body(v_ref, src_ref, skip_ref, up_ref, down_ref, back_ref, rowt_ref, *rest):
        if want_rows:
            out_ref, rows_ref, turned, zs, made = rest
        else:
            out_ref, turned, zs = rest
        i = pl.program_id(0)

        @pl.when(i == 0)
        def _():
            load_rows(src_ref, turned, C, CP, H)

        at = pl.ds(pl.multiple_of(i * HB * CP, HB * CP), HB * CP)
        zs[...] = dot(turned[at, :].astype(BF), back_ref[...]) * (1.0 / length)
        for j in range(0, HB, G):
            vh = v_ref[j:j + G].reshape(G * CP, W)
            z = zs[j * CP:(j + G) * CP, :] + dot(skip_ref[...], vh)
            y = gate(z).astype(BF)
            act = gate(dot(up_ref[...], y)).astype(BF)
            out_ref[j:j + G] = (vh.astype(F32) + dot(down_ref[...], act)).astype(BF).reshape(G, CP, W)
        if want_rows:
            made[at, :] = dot(out_ref[...].reshape(HB * CP, W), rowt_ref[...])

            @pl.when(i == steps - 1)
            def _():
                store_rows(made, rows_ref, C, CP, H)

    block = pl.BlockSpec((HB, CP, W), lambda i: (i, 0, 0))
    outs = ([block], [jax.ShapeDtypeStruct(v.shape, BF)])
    scratch = [pltpu.VMEM((H * CP, J), F32), pltpu.VMEM((HB * CP, W), F32)]
    if want_rows:
        outs[0].append(same((J, C * H)))
        outs[1].append(jax.ShapeDtypeStruct((J, C * H), BF))
        scratch.append(pltpu.VMEM((H * CP, J), F32))
    return call(
        body, (steps,),
        [block, same(src.shape), same(skip.shape), same(up.shape), same(down.shape), same(back.shape), same(row_t.shape)],
        outs, scratch, cost=(4 * H * CP * W * (F + J), 4 * H * CP * W),
    )(v, src, skip, up, down, back, row_t)


def field_backward(v, g, src, skip, up, down, up_t, down_t, back, back_t, length):
    H, CP, W = v.shape
    J = back.shape[0]
    C = src.shape[1] // H
    F = up.shape[0] // G
    steps = H // HB

    def body(v_ref, g_ref, src_ref, skip_ref, up_ref, down_ref, upt_ref, downt_ref, back_ref, backt_ref,
             gz_ref, rows_ref, gskip_ref, gup_ref, gdown_ref, turned, zs, made):
        i = pl.program_id(0)

        @pl.when(i == 0)
        def _():
            load_rows(src_ref, turned, C, CP, H)
            gskip_ref[...] = jnp.zeros_like(gskip_ref)
            gup_ref[...] = jnp.zeros_like(gup_ref)
            gdown_ref[...] = jnp.zeros_like(gdown_ref)

        at = pl.ds(pl.multiple_of(i * HB * CP, HB * CP), HB * CP)
        zs[...] = dot(turned[at, :].astype(BF), back_ref[...]) * (1.0 / length)
        for j in range(0, HB, G):
            vh = v_ref[j:j + G].reshape(G * CP, W)
            gh = g_ref[j:j + G].reshape(G * CP, W)
            z = zs[j * CP:(j + G) * CP, :] + dot(skip_ref[...], vh)
            y, y_slope = gate_pair(z)
            y = y.astype(BF)
            act, act_slope = gate_pair(dot(up_ref[...], y))
            act = act.astype(BF)
            grad_hidden = (dot(downt_ref[...], gh) * act_slope).astype(BF)
            gz = (dot(upt_ref[...], grad_hidden) * y_slope).astype(BF)
            gz_ref[j:j + G] = gz.reshape(G, CP, W)
            gdown_ref[...] += dot(act, gh, 1, 1)
            gup_ref[...] += dot(grad_hidden, y, 1, 1)
            gskip_ref[...] += dot(gz, vh, 1, 1)

        made[at, :] = dot(gz_ref[...].reshape(HB * CP, W), backt_ref[...]) * (1.0 / length)

        @pl.when(i == steps - 1)
        def _():
            store_rows(made, rows_ref, C, CP, H)

    block = pl.BlockSpec((HB, CP, W), lambda i: (i, 0, 0))
    args = (v, g, src, skip, up, down, up_t, down_t, back, back_t)
    small = [(G * CP, G * CP), (G * F, G * CP), (G * F, G * CP)]
    return call(
        body, (steps,),
        [block, block] + [same(a.shape) for a in args[2:]],
        ([block, same((J, C * H))] + [same(s) for s in small],
         [jax.ShapeDtypeStruct(v.shape, BF), jax.ShapeDtypeStruct((J, C * H), BF)]
         + [jax.ShapeDtypeStruct(s, F32) for s in small]),
        [pltpu.VMEM((H * CP, J), F32), pltpu.VMEM((HB * CP, W), F32), pltpu.VMEM((H * CP, J), F32)],
        cost=(8 * H * CP * W * (F + J), 6 * H * CP * W),
    )(*args)


def field_grad(g, gz, src, skip_t, row):
    H, CP, W = g.shape
    J = row.shape[0]
    C = src.shape[1] // H
    steps = H // HB

    def body(g_ref, gz_ref, src_ref, skipt_ref, row_ref, out_ref, turned, zs):
        i = pl.program_id(0)

        @pl.when(i == 0)
        def _():
            load_rows(src_ref, turned, C, CP, H)

        at = pl.ds(pl.multiple_of(i * HB * CP, HB * CP), HB * CP)
        zs[...] = dot(turned[at, :].astype(BF), row_ref[...])

        for j in range(0, HB, G):
            gh = g_ref[j:j + G].reshape(G * CP, W).astype(F32)
            gz = gz_ref[j:j + G].reshape(G * CP, W)
            out_ref[j:j + G] = (gh + dot(skipt_ref[...], gz) + zs[j * CP:(j + G) * CP, :]).astype(BF).reshape(G, CP, W)

    block = pl.BlockSpec((HB, CP, W), lambda i: (i, 0, 0))
    return call(
        body, (steps,),
        [block, block, same(src.shape), same(skip_t.shape), same(row.shape)],
        (block, jax.ShapeDtypeStruct(g.shape, BF)),
        [pltpu.VMEM((H * CP, J), F32), pltpu.VMEM((HB * CP, W), F32)],
        cost=(2 * H * CP * W * J, 6 * H * CP * W),
    )(g, gz, src, skip_t, row)


def repeated(weight):
    L, a, b = weight.shape
    eye = jnp.eye(G, dtype=bool)[None, :, None, :, None]
    return jnp.where(eye, weight[:, None, :, None, :], jnp.zeros((), weight.dtype)).reshape(L, G * a, G * b)


def own_blocks(total):
    a, b = total.shape
    return jnp.einsum("iaib->ab", total.reshape(G, a // G, G, b // G))


def exchanged(spectra, groups):
    blocks = spectra.reshape(groups, spectra.size // spectra.shape[-1] // groups, spectra.shape[-1])
    return lax.all_to_all(blocks, "slab", split_axis=0, concat_axis=0, tiled=True)


def fast_shards(emitted, returned, stash, skip_w, up_w, down_w, spec_w):
    _, C, H, W = emitted.shape
    L = spec_w.shape[1]
    S = lax.axis_size("slab")
    mode_count = spec_w.shape[2] * S
    CP = -(-C // 16) * 16
    row, row_t, back, back_t, col, col_t = fast_tables(W, mode_count, S)
    spec = spec_w[0].transpose(0, 1, 3, 4, 2, 5).reshape(L, spec_w.shape[2], C, 2 * C, spec_w.shape[6])
    pad = CP - C
    skip = jnp.pad(skip_w[0], ((0, 0), (0, pad), (0, pad)))
    up = jnp.pad(up_w[0], ((0, 0), (0, 0), (0, pad)))
    down = jnp.pad(down_w[0], ((0, 0), (0, pad), (0, 0)))
    turn = lambda a: jnp.swapaxes(a, 1, 2)
    skip_t, up_t, down_t = repeated(turn(skip)), repeated(turn(up)), repeated(turn(down))
    skip, up, down = repeated(skip), repeated(up), repeated(down)
    size = lax.axis_size("section")
    lined = lambda f: jnp.pad(jnp.swapaxes(f, 0, 1), ((0, 0), (0, pad), (0, 0)))
    plain = lambda f: jnp.swapaxes(f[:, :C], 0, 1)
    flat = lambda a: a.reshape(-1, a.shape[-1])

    rows_a = passed_along(first_rows(emitted[0], row), "section", 1)
    rows_k = passed_along(first_rows(stash[0], row), "section", size // 2)
    rows_a, rows_k, emitted = lax.optimization_barrier((rows_a, rows_k, emitted))
    ahead = passed_along(emitted[0], "section", 1)
    rows_a, rows_k = exchanged(rows_a, S), exchanged(rows_k, S)
    ahead, stash = lax.optimization_barrier((ahead, stash))
    kept = passed_along(stash[0], "section", size // 2)
    kept, returned = lax.optimization_barrier((kept, returned))
    top = passed_along(returned[0], "section", -1)

    ahead = lined(ahead)
    for l in range(L):
        mixed, _ = modes_forward(spec, l, rows_a, col, col_t, W)
        made = field_forward(ahead, flat(exchanged(mixed, S)), skip[l], up[l], down[l], back, row_t, W, l < L - 1)
        ahead = made[0]
        if l < L - 1:
            rows_a = exchanged(made[1], S)
    sent = plain(ahead)

    kept = lined(kept)
    saved = []
    for l in range(L):
        mixed, modes = modes_forward(spec, l, rows_k, col, col_t, W)
        arrived = flat(exchanged(mixed, S))
        saved.append((kept, arrived, modes))
        if l < L - 1:
            kept, rows_k = field_forward(kept, arrived, skip[l], up[l], down[l], back, row_t, W, True)
            rows_k = exchanged(rows_k, S)
    g = lined(top)
    spec_grad = None
    skips, ups, downs = [], [], []
    for l in reversed(range(L)):
        v, arrived, modes = saved[l]
        gz, rows, gs, gu, gd = field_backward(v, g, arrived, skip[l], up[l], down[l], up_t[l], down_t[l], back, back_t, W)
        mixed, spec_grad = modes_backward(spec, l, exchanged(rows, S), modes, col, col_t, W, spec_grad)
        g = field_grad(g, gz, flat(exchanged(mixed, S)), skip_t[l], row)
        skips.insert(0, own_blocks(gs)[:C, :C])
        ups.insert(0, own_blocks(gu)[:, :C])
        downs.insert(0, own_blocks(gd)[:, :C].T)
    parts = [jnp.stack(skips), jnp.stack(ups), jnp.stack(downs)]
    flat_parts = jnp.concatenate([a.reshape(-1) for a in parts]) / W
    size_up = -(-flat_parts.size // 1024) * 1024
    packed = jnp.pad(flat_parts, (0, size_up - flat_parts.size)).reshape(1, -1, 128)
    everyone = lax.all_to_all(jnp.broadcast_to(packed, (S,) + packed.shape[1:]), "slab", 0, 0, tiled=True)
    total = jnp.sum(everyone, axis=0).reshape(-1)
    summed, at = [], 0
    for a in parts:
        summed.append(total[at:at + a.size].reshape(a.shape))
        at += a.size
    spec_grad = spec_grad.reshape(L, spec_w.shape[2], C, C, 2, spec_w.shape[6]).transpose(0, 1, 4, 2, 3, 5)
    return (sent[None], plain(g)[None], summed[0][None], summed[1][None], summed[2][None], spec_grad[None])


def work(*args):
    H = args[0].shape[2]
    K = args[6].shape[2]
    if H % 128 == 0 and K % 16 == 0 and H % HB == 0 and args[6].shape[6] == 128 and 2 * K * lax.axis_size("slab") == 128:
        return fast_shards(*args)
    return shards(*args)


def solution(mesh):
    placed = (
        P("section", None, "slab", None),
        P("section", None, "slab", None),
        P("section", None, "slab", None),
        P("section", None, None, None),
        P("section", None, None, None),
        P("section", None, None, None),
        P("section", None, "slab", None, None, None, None),
    )
    return jax.shard_map(
        work,
        mesh=mesh,
        in_specs=placed,
        out_specs=(
            P("section", None, "slab", None),
            P("section", None, "slab", None),
            P("section", None, None, None),
            P("section", None, None, None),
            P("section", None, None, None),
            P("section", None, "slab", None, None, None, None),
        ),
        check_vma=False,
    )
```

```python
import jax
import jax.numpy as jnp
import numpy as np
from jax import lax
from jax.experimental import pallas as pl
from jax.experimental.pallas import tpu as pltpu
from jax.sharding import PartitionSpec as P

M = 64
LAYERS = 2


root_two_pi = 0.7978845608028654
cubic_coef = 0.044715


def from_partner(array, axis, stride):
    return lax.ppermute(array, axis, [(i, i ^ 1 << stride) for i in range(lax.axis_size(axis))])


def passed_along(block, axis, distance):
    devices = range(lax.axis_size(axis))
    route = [((i - distance) % len(devices), i) for i in devices]
    return lax.ppermute(block, axis, route)


def smooth_gate(values):
    return (
        0.5
        * values
        * (1.0 + jnp.tanh(root_two_pi * (values + cubic_coef * values * values * values)))
    )


def gate_slope(values):
    tangent = jnp.tanh(root_two_pi * (values + cubic_coef * values * values * values))
    return 0.5 * (1.0 + tangent) + 0.5 * values * (1.0 - tangent * tangent) * root_two_pi * (
        1.0 + 3.0 * cubic_coef * values * values
    )


def angles(left_idx, right_idx, length):
    product_idx = left_idx[:, None] * right_idx[None, :] % length
    return 2.0 * jnp.pi / length * product_idx.astype(jnp.float32)


def tables(length, mode_count):
    cell_idx = jnp.arange(length, dtype=jnp.int32)
    low_modes = jnp.arange(mode_count, dtype=jnp.int32)
    both_modes = jnp.concatenate([low_modes, low_modes + (length - mode_count)])
    along_w = angles(cell_idx, low_modes, length)
    cos_w = jnp.cos(along_w)
    sin_w = jnp.sin(along_w)
    row_table = jnp.stack([cos_w, -sin_w], axis=1).astype(jnp.bfloat16)
    weight = jnp.where(low_modes == 0, 1.0, 2.0).astype(jnp.float32)[:, None]
    back_table = jnp.stack([weight * cos_w.T, -weight * sin_w.T], axis=1).astype(jnp.bfloat16)
    along_h = angles(cell_idx, both_modes, length)
    cos_h = jnp.cos(along_h)
    sin_h = jnp.sin(along_h)
    col_table = jnp.stack(
        [jnp.stack([cos_h, -sin_h], axis=1), jnp.stack([sin_h, cos_h], axis=1)], axis=0
    ).astype(jnp.bfloat16)
    return (row_table, back_table, col_table)


def product(form, left, right):
    return jnp.einsum(form, left, right, preferred_element_type=jnp.float32)


def to_modes(row_spec):
    return lax.all_to_all(row_spec, "slab", split_axis=0, concat_axis=3, tiled=True)


def to_rows(back_spec):
    return lax.all_to_all(back_spec, "slab", split_axis=3, concat_axis=0, tiled=True)


def fetch_saved(saved_input):
    top_bit = lax.axis_size("section").bit_length() - 1
    return from_partner(saved_input, "section", top_bit - 1)


def mix_modes(spec_layer, mode_spec):
    real_weight = spec_layer[:, 0]
    imag_weight = spec_layer[:, 1]
    real_mode = mode_spec[:, :, 0]
    imag_mode = mode_spec[:, :, 1]
    out_real = product("koix,kix->kox", real_weight, real_mode) - product(
        "koix,kix->kox", imag_weight, imag_mode
    )
    out_imag = product("koix,kix->kox", real_weight, imag_mode) + product(
        "koix,kix->kox", imag_weight, real_mode
    )
    return jnp.stack([out_real, out_imag], axis=1)


def mix_adjoint(spec_layer, mode_spec, grad_mixed):
    real_weight = spec_layer[:, 0]
    imag_weight = spec_layer[:, 1]
    real_mode = mode_spec[:, :, 0]
    imag_mode = mode_spec[:, :, 1]
    real_grad = grad_mixed[:, 0]
    imag_grad = grad_mixed[:, 1]
    grad_real = product("koix,kox->kix", real_weight, real_grad) + product(
        "koix,kox->kix", imag_weight, imag_grad
    )
    grad_imag = product("koix,kox->kix", real_weight, imag_grad) - product(
        "koix,kox->kix", imag_weight, real_grad
    )
    spec_real = product("kox,kix->koix", real_grad, real_mode) + product(
        "kox,kix->koix", imag_grad, imag_mode
    )
    spec_imag = product("kox,kix->koix", imag_grad, real_mode) - product(
        "kox,kix->koix", real_grad, imag_mode
    )
    return (jnp.stack([grad_real, grad_imag], axis=2), jnp.stack([spec_real, spec_imag], axis=1))


def layer_forward(activity, skip_layer, up_layer, down_layer, spec_layer, table_set):
    row_table, back_table, col_table = table_set
    length = activity.shape[2]
    row_spec = to_modes(product("chw,wpk->kpch", activity, row_table).astype(jnp.bfloat16))
    mode_spec = (product("kpch,phqx->kcqx", row_spec, col_table) / length).astype(jnp.bfloat16)
    mixed_modes = mix_modes(spec_layer, mode_spec).astype(jnp.bfloat16)
    back_spec = to_rows(product("kqcx,phqx->kpch", mixed_modes, col_table).astype(jnp.bfloat16))
    spectral = product("kpch,kpw->chw", back_spec, back_table) / length
    pre_act = spectral + product("oc,chw->ohw", skip_layer, activity)
    gated_act = smooth_gate(pre_act).astype(jnp.bfloat16)
    hidden = product("fc,chw->fhw", up_layer, gated_act)
    inner_act = smooth_gate(hidden).astype(jnp.bfloat16)
    result = (activity.astype(jnp.float32) + product("cf,fhw->chw", down_layer, inner_act)).astype(
        jnp.bfloat16
    )
    return (result, (activity, mode_spec, pre_act, gated_act, hidden, inner_act))


def layer_backward(grad_out, saved_act, skip_layer, up_layer, down_layer, spec_layer, table_set):
    row_table, back_table, col_table = table_set
    activity, mode_spec, pre_act, gated_act, hidden, inner_act = saved_act
    length = activity.shape[2]
    grad_inner = product("cf,chw->fhw", down_layer, grad_out)
    grad_down = product("chw,fhw->cf", grad_out, inner_act) / length
    grad_hidden = (grad_inner * gate_slope(hidden)).astype(jnp.bfloat16)
    grad_gated = product("fc,fhw->chw", up_layer, grad_hidden)
    grad_up = product("fhw,chw->fc", grad_hidden, gated_act) / length
    grad_pre = (grad_gated * gate_slope(pre_act)).astype(jnp.bfloat16)
    grad_skip = product("ohw,chw->oc", grad_pre, activity) / length
    grad_back = to_modes(
        (product("chw,kpw->kpch", grad_pre, back_table) / length).astype(jnp.bfloat16)
    )
    grad_mixed = product("kpch,phqx->kqcx", grad_back, col_table).astype(jnp.bfloat16)
    grad_modes, grad_spec = mix_adjoint(spec_layer, mode_spec, grad_mixed)
    grad_rows = to_rows(
        (product("kcqx,phqx->kpch", grad_modes.astype(jnp.bfloat16), col_table) / length).astype(
            jnp.bfloat16
        )
    )
    grad_field = (
        grad_out.astype(jnp.float32)
        + product("oc,ohw->chw", skip_layer, grad_pre)
        + product("kpch,wpk->chw", grad_rows, row_table)
    )
    return (grad_field.astype(jnp.bfloat16), grad_skip, grad_up, grad_down, grad_spec)


def shards(emitted, returned, stash, skip_w, up_w, down_w, spec_w):
    length = emitted.shape[3]
    table_set = tables(length, M)
    skip_section = skip_w[0]
    up_section = up_w[0]
    down_section = down_w[0]
    spec_section = spec_w[0]
    ahead_input = passed_along(emitted[0], "section", 1)
    top_grad = passed_along(returned[0], "section", -1)
    kept_input = fetch_saved(stash[0])
    activity = ahead_input
    for layer_idx in range(LAYERS):
        activity, unused_keep = layer_forward(
            activity,
            skip_section[layer_idx],
            up_section[layer_idx],
            down_section[layer_idx],
            spec_section[layer_idx],
            table_set,
        )
    sent_out = activity
    activity = kept_input
    saved_list = []
    for layer_idx in range(LAYERS):
        activity, layer_keep = layer_forward(
            activity,
            skip_section[layer_idx],
            up_section[layer_idx],
            down_section[layer_idx],
            spec_section[layer_idx],
            table_set,
        )
        saved_list.append(layer_keep)
    grad_now = top_grad
    skip_list, up_list, down_list, spec_list = ([], [], [], [])
    for layer_idx in reversed(range(LAYERS)):
        grad_now, grad_skip, grad_up, grad_down, grad_spec = layer_backward(
            grad_now,
            saved_list[layer_idx],
            skip_section[layer_idx],
            up_section[layer_idx],
            down_section[layer_idx],
            spec_section[layer_idx],
            table_set,
        )
        skip_list.insert(0, grad_skip)
        up_list.insert(0, grad_up)
        down_list.insert(0, grad_down)
        spec_list.insert(0, grad_spec)
    summed = lax.psum((jnp.stack(skip_list), jnp.stack(up_list), jnp.stack(down_list)), "slab")
    return (
        sent_out[None],
        grad_now[None],
        summed[0][None],
        summed[1][None],
        summed[2][None],
        jnp.stack(spec_list)[None],
    )


BF = jnp.bfloat16
F32 = jnp.float32
VM = 60 * 1024 * 1024


def fast_tables(length, mode_count, groups):
    ang = lambda a, b: (np.float32(2.0 * np.pi / length) * ((a[:, None] * b[None, :]) % length).astype(np.float32))
    cells = np.arange(length)
    low = np.arange(mode_count)
    both = np.concatenate([low, low + (length - mode_count)])
    along = ang(low, cells)
    cos_w, sin_w = np.cos(along), np.sin(along)
    weight = np.where(low == 0, 1.0, 2.0).astype(np.float32)[:, None]

    def grouped(a, b):
        a = a.reshape(groups, 1, mode_count // groups, length)
        b = b.reshape(groups, 1, mode_count // groups, length)
        return np.concatenate([a, b], axis=1).reshape(2 * mode_count, length)

    row = grouped(cos_w, -sin_w)
    back = grouped(weight * cos_w, -weight * sin_w)
    along_h = ang(cells, both)
    cos_h, sin_h = np.cos(along_h), np.sin(along_h)
    col = np.stack([np.concatenate([cos_h, -sin_h], 1), np.concatenate([sin_h, cos_h], 1)], 0)
    modes = col.shape[2]
    col = col.reshape(2, groups, length // groups, modes).transpose(1, 0, 2, 3).reshape(2 * length, modes)
    made = lambda t: jnp.asarray(t.astype(BF))
    return made(row), made(row.T), made(back), made(back.T), made(col), made(col.T)


def call(body, grid, ins, outs, scratch, aliases=None, cost=(0, 0)):
    return pl.pallas_call(
        body,
        grid=grid,
        in_specs=ins,
        out_specs=outs[0],
        out_shape=outs[1],
        scratch_shapes=scratch,
        input_output_aliases=aliases or {},
        compiler_params=pltpu.CompilerParams(
            dimension_semantics=("arbitrary",) * len(grid), vmem_limit_bytes=VM
        ),
        cost_estimate=pl.CostEstimate(flops=cost[0], bytes_accessed=cost[1], transcendentals=0),
    )


def same(shape):
    return pl.BlockSpec(shape, lambda i: (0,) * len(shape))


def dot(a, b, ca=1, cb=0):
    return lax.dot_general(a, b, (((ca,), (cb,)), ((), ())), preferred_element_type=F32)


def first_rows(field, row):
    C, H, W = field.shape
    J = row.shape[0]
    cb = next(n for n in (5, 4, 2, 1) if C % n == 0)

    def body(v_ref, row_ref, out_ref):
        v = v_ref[...].reshape(cb * H, W)
        out_ref[...] = dot(row_ref[...], v, 1, 1).astype(BF)

    return call(
        body, (C // cb,),
        [pl.BlockSpec((cb, H, W), lambda i: (i, 0, 0)), same((J, W))],
        (pl.BlockSpec((J, cb * H), lambda i: (0, i)), jax.ShapeDtypeStruct((J, C * H), BF)),
        [], cost=(2 * J * C * H * W, 2 * C * H * W),
    )(field, row)


def gather_modes(src_ref, lhs, C, S, K, H):
    for c in range(C):
        for s in range(S):
            for p in range(2):
                j = s * 2 + p
                lhs[c * K:(c + 1) * K, j * H:(j + 1) * H] = src_ref[s, p * K:(p + 1) * K, c * H:(c + 1) * H]


def spread_modes(wide, out_ref, C, S, K, H):
    for c in range(C):
        for s in range(S):
            for p in range(2):
                j = s * 2 + p
                out_ref[s, p * K:(p + 1) * K, c * H:(c + 1) * H] = wide[c * K:(c + 1) * K, j * H:(j + 1) * H].astype(BF)


def split_parts(wide, parts):
    rows, X = parts.shape
    parts[:rows // 2, :] = wide[:, :X]
    parts[rows // 2:, :] = wide[:, X:]


def joined_parts(parts):
    rows = parts.shape[0] // 2
    return jnp.concatenate([parts[:rows, :], parts[rows:, :]], axis=1).astype(BF)


def weave(pair, real, imag, C):
    even, odd = pl.ds(0, C, stride=2), pl.ds(1, C, stride=2)
    pair[0, even, :] = real
    pair[0, odd, :] = -imag
    pair[1, even, :] = imag
    pair[1, odd, :] = real


def modes_forward(spec, layer, src, col, col_t, length):
    _, K, C, _, X = spec.shape
    S, _, CH = src.shape
    H = CH // C

    def body(r_ref, src_ref, col_ref, colt_ref, out_ref, x_ref, lhs, xs, ys, pair):
        k = pl.program_id(0)

        @pl.when(k == 0)
        def _():
            gather_modes(src_ref, lhs, C, S, K, H)
            x_ref[...] = (dot(lhs[...], col_ref[...]) * (1.0 / length)).astype(BF)
            split_parts(x_ref[...].astype(F32), xs)

        real, imag = pl.ds(k, C, stride=K), pl.ds(C * K + k, C, stride=K)
        weave(pair, xs[real, :], xs[imag, :], C)
        held = r_ref[0, 0].astype(F32)
        ys[real, :] = jnp.sum(held * pair[0][None], axis=1)
        ys[imag, :] = jnp.sum(held * pair[1][None], axis=1)

        @pl.when(k == K - 1)
        def _():
            spread_modes(dot(joined_parts(ys), colt_ref[...]), out_ref, C, S, K, H)

    J = col.shape[0]
    return call(
        body, (K,),
        [pl.BlockSpec((1, 1, C, 2 * C, X), lambda i: (layer, i, 0, 0, 0)), same(src.shape), same(col.shape), same(col_t.shape)],
        ([same(src.shape), same((C * K, 2 * X))],
         [jax.ShapeDtypeStruct(src.shape, BF), jax.ShapeDtypeStruct((C * K, 2 * X), BF)]),
        [pltpu.VMEM((C * K, J), BF), pltpu.VMEM((2 * C * K, X), F32), pltpu.VMEM((2 * C * K, X), F32), pltpu.VMEM((2, 2 * C, X), F32)],
        cost=(8 * C * K * J * X, 8 * K * C * C * X),
    )(spec, src, col, col_t)


def modes_backward(spec, layer, src, kept_modes, col, col_t, length, held):
    L, K, C, _, X = spec.shape
    S, _, CH = src.shape
    H = CH // C

    def body(r_ref, src_ref, m_ref, col_ref, colt_ref, *rest):
        out_ref, grad_ref, lhs, xs, gs, ys, pair = rest[-7:]
        k = pl.program_id(0)

        @pl.when(k == 0)
        def _():
            gather_modes(src_ref, lhs, C, S, K, H)
            split_parts(dot(lhs[...], col_ref[...]).astype(BF).astype(F32), gs)
            split_parts(m_ref[...].astype(F32), xs)

        real, imag = pl.ds(k, C, stride=K), pl.ds(C * K + k, C, stride=K)
        gr = gs[real, :][:, None, :]
        gi = gs[imag, :][:, None, :]
        weave(pair, xs[real, :], xs[imag, :], C)
        grad_ref[0, 0] = gr * pair[0][None] + gi * pair[1][None]
        held = r_ref[0, 0].astype(F32)
        pair[0] = jnp.sum(held * gr, axis=0)
        pair[1] = jnp.sum(held * gi, axis=0)
        even, odd = pl.ds(0, C, stride=2), pl.ds(1, C, stride=2)
        ys[real, :] = pair[0, even, :] + pair[1, odd, :]
        ys[imag, :] = pair[1, even, :] - pair[0, odd, :]

        @pl.when(k == K - 1)
        def _():
            spread_modes(dot(joined_parts(ys), colt_ref[...]) * (1.0 / length), out_ref, C, S, K, H)

    J = col.shape[0]
    block = pl.BlockSpec((1, 1, C, 2 * C, X), lambda i: (layer, i, 0, 0, 0))
    ins = [block, same(src.shape), same(kept_modes.shape), same(col.shape), same(col_t.shape)]
    args = [spec, src, kept_modes, col, col_t]
    aliases = {}
    if held is not None:
        ins.append(pl.BlockSpec(memory_space=pl.ANY))
        args.append(held)
        aliases = {5: 1}
    return call(
        body, (K,), ins,
        ([same(src.shape), block], [jax.ShapeDtypeStruct(src.shape, BF), jax.ShapeDtypeStruct(spec.shape, F32)]),
        [pltpu.VMEM((C * K, J), BF)] + [pltpu.VMEM((2 * C * K, X), F32)] * 3 + [pltpu.VMEM((2, 2 * C, X), F32)],
        aliases, cost=(8 * C * K * J * X, 16 * K * C * C * X),
    )(*args)


def load_rows(src_ref, turned, C, CP, H):
    J = turned.shape[1]
    turned[...] = jnp.zeros_like(turned)
    for c in range(C):
        tile = src_ref[:, c * H:(c + 1) * H].astype(F32)
        turned[pl.ds(c, H, stride=CP), :] = tile.T


def store_rows(turned, out_ref, C, CP, H):
    for c in range(C):
        tile = turned[pl.ds(c, H, stride=CP), :]
        out_ref[:, c * H:(c + 1) * H] = tile.T.astype(BF)


def tanh_of(t, t2):
    return jnp.tanh(t * (root_two_pi + (root_two_pi * cubic_coef) * t2))


def gate(t):
    half = 0.5 * t
    return half + half * tanh_of(t, t * t)


def gate_pair(t):
    t2 = t * t
    th = tanh_of(t, t2)
    near = 0.5 + 0.5 * th
    half = 0.5 * t
    slope = near + half * (1.0 - th * th) * (root_two_pi + (3.0 * cubic_coef * root_two_pi) * t2)
    return t * near, slope


HB = 16
G = 8


def field_forward(v, src, skip, up, down, back, row_t, length, want_rows):
    H, CP, W = v.shape
    J = back.shape[0]
    C = src.shape[1] // H
    F = up.shape[0] // G
    steps = H // HB

    def body(v_ref, src_ref, skip_ref, up_ref, down_ref, back_ref, rowt_ref, *rest):
        if want_rows:
            out_ref, rows_ref, turned, zs, made = rest
        else:
            out_ref, turned, zs = rest
        i = pl.program_id(0)

        @pl.when(i == 0)
        def _():
            load_rows(src_ref, turned, C, CP, H)

        at = pl.ds(pl.multiple_of(i * HB * CP, HB * CP), HB * CP)
        zs[...] = dot(turned[at, :].astype(BF), back_ref[...]) * (1.0 / length)
        for j in range(0, HB, G):
            vh = v_ref[j:j + G].reshape(G * CP, W)
            z = zs[j * CP:(j + G) * CP, :] + dot(skip_ref[...], vh)
            y = gate(z).astype(BF)
            act = gate(dot(up_ref[...], y)).astype(BF)
            out_ref[j:j + G] = (vh.astype(F32) + dot(down_ref[...], act)).astype(BF).reshape(G, CP, W)
        if want_rows:
            made[at, :] = dot(out_ref[...].reshape(HB * CP, W), rowt_ref[...])

            @pl.when(i == steps - 1)
            def _():
                store_rows(made, rows_ref, C, CP, H)

    block = pl.BlockSpec((HB, CP, W), lambda i: (i, 0, 0))
    outs = ([block], [jax.ShapeDtypeStruct(v.shape, BF)])
    scratch = [pltpu.VMEM((H * CP, J), F32), pltpu.VMEM((HB * CP, W), F32)]
    if want_rows:
        outs[0].append(same((J, C * H)))
        outs[1].append(jax.ShapeDtypeStruct((J, C * H), BF))
        scratch.append(pltpu.VMEM((H * CP, J), F32))
    return call(
        body, (steps,),
        [block, same(src.shape), same(skip.shape), same(up.shape), same(down.shape), same(back.shape), same(row_t.shape)],
        outs, scratch, cost=(4 * H * CP * W * (F + J), 4 * H * CP * W),
    )(v, src, skip, up, down, back, row_t)


def field_backward(v, g, src, skip, up, down, up_t, down_t, back, back_t, length):
    H, CP, W = v.shape
    J = back.shape[0]
    C = src.shape[1] // H
    F = up.shape[0] // G
    steps = H // HB

    def body(v_ref, g_ref, src_ref, skip_ref, up_ref, down_ref, upt_ref, downt_ref, back_ref, backt_ref,
             gz_ref, rows_ref, gskip_ref, gup_ref, gdown_ref, turned, zs, made):
        i = pl.program_id(0)

        @pl.when(i == 0)
        def _():
            load_rows(src_ref, turned, C, CP, H)
            gskip_ref[...] = jnp.zeros_like(gskip_ref)
            gup_ref[...] = jnp.zeros_like(gup_ref)
            gdown_ref[...] = jnp.zeros_like(gdown_ref)

        at = pl.ds(pl.multiple_of(i * HB * CP, HB * CP), HB * CP)
        zs[...] = dot(turned[at, :].astype(BF), back_ref[...]) * (1.0 / length)
        for j in range(0, HB, G):
            vh = v_ref[j:j + G].reshape(G * CP, W)
            gh = g_ref[j:j + G].reshape(G * CP, W)
            z = zs[j * CP:(j + G) * CP, :] + dot(skip_ref[...], vh)
            y, y_slope = gate_pair(z)
            y = y.astype(BF)
            act, act_slope = gate_pair(dot(up_ref[...], y))
            act = act.astype(BF)
            grad_hidden = (dot(downt_ref[...], gh) * act_slope).astype(BF)
            gz = (dot(upt_ref[...], grad_hidden) * y_slope).astype(BF)
            gz_ref[j:j + G] = gz.reshape(G, CP, W)
            gdown_ref[...] += dot(act, gh, 1, 1)
            gup_ref[...] += dot(grad_hidden, y, 1, 1)
            gskip_ref[...] += dot(gz, vh, 1, 1)

        made[at, :] = dot(gz_ref[...].reshape(HB * CP, W), backt_ref[...]) * (1.0 / length)

        @pl.when(i == steps - 1)
        def _():
            store_rows(made, rows_ref, C, CP, H)

    block = pl.BlockSpec((HB, CP, W), lambda i: (i, 0, 0))
    args = (v, g, src, skip, up, down, up_t, down_t, back, back_t)
    small = [(G * CP, G * CP), (G * F, G * CP), (G * F, G * CP)]
    return call(
        body, (steps,),
        [block, block] + [same(a.shape) for a in args[2:]],
        ([block, same((J, C * H))] + [same(s) for s in small],
         [jax.ShapeDtypeStruct(v.shape, BF), jax.ShapeDtypeStruct((J, C * H), BF)]
         + [jax.ShapeDtypeStruct(s, F32) for s in small]),
        [pltpu.VMEM((H * CP, J), F32), pltpu.VMEM((HB * CP, W), F32), pltpu.VMEM((H * CP, J), F32)],
        cost=(8 * H * CP * W * (F + J), 6 * H * CP * W),
    )(*args)


def field_grad(g, gz, src, skip_t, row):
    H, CP, W = g.shape
    J = row.shape[0]
    C = src.shape[1] // H
    steps = H // HB

    def body(g_ref, gz_ref, src_ref, skipt_ref, row_ref, out_ref, turned, zs):
        i = pl.program_id(0)

        @pl.when(i == 0)
        def _():
            load_rows(src_ref, turned, C, CP, H)

        at = pl.ds(pl.multiple_of(i * HB * CP, HB * CP), HB * CP)
        zs[...] = dot(turned[at, :].astype(BF), row_ref[...])

        for j in range(0, HB, G):
            gh = g_ref[j:j + G].reshape(G * CP, W).astype(F32)
            gz = gz_ref[j:j + G].reshape(G * CP, W)
            out_ref[j:j + G] = (gh + dot(skipt_ref[...], gz) + zs[j * CP:(j + G) * CP, :]).astype(BF).reshape(G, CP, W)

    block = pl.BlockSpec((HB, CP, W), lambda i: (i, 0, 0))
    return call(
        body, (steps,),
        [block, block, same(src.shape), same(skip_t.shape), same(row.shape)],
        (block, jax.ShapeDtypeStruct(g.shape, BF)),
        [pltpu.VMEM((H * CP, J), F32), pltpu.VMEM((HB * CP, W), F32)],
        cost=(2 * H * CP * W * J, 6 * H * CP * W),
    )(g, gz, src, skip_t, row)


def repeated(weight):
    L, a, b = weight.shape
    eye = jnp.eye(G, dtype=bool)[None, :, None, :, None]
    return jnp.where(eye, weight[:, None, :, None, :], jnp.zeros((), weight.dtype)).reshape(L, G * a, G * b)


def own_blocks(total):
    a, b = total.shape
    return jnp.einsum("iaib->ab", total.reshape(G, a // G, G, b // G))


def exchanged(spectra, groups):
    blocks = spectra.reshape(groups, spectra.size // spectra.shape[-1] // groups, spectra.shape[-1])
    return lax.all_to_all(blocks, "slab", split_axis=0, concat_axis=0, tiled=True)


def fast_shards(emitted, returned, stash, skip_w, up_w, down_w, spec_w):
    _, C, H, W = emitted.shape
    L = spec_w.shape[1]
    S = lax.axis_size("slab")
    mode_count = spec_w.shape[2] * S
    CP = -(-C // 16) * 16
    row, row_t, back, back_t, col, col_t = fast_tables(W, mode_count, S)
    spec = spec_w[0].transpose(0, 1, 3, 4, 2, 5).reshape(L, spec_w.shape[2], C, 2 * C, spec_w.shape[6])
    pad = CP - C
    skip = jnp.pad(skip_w[0], ((0, 0), (0, pad), (0, pad)))
    up = jnp.pad(up_w[0], ((0, 0), (0, 0), (0, pad)))
    down = jnp.pad(down_w[0], ((0, 0), (0, pad), (0, 0)))
    turn = lambda a: jnp.swapaxes(a, 1, 2)
    skip_t, up_t, down_t = repeated(turn(skip)), repeated(turn(up)), repeated(turn(down))
    skip, up, down = repeated(skip), repeated(up), repeated(down)
    size = lax.axis_size("section")
    lined = lambda f: jnp.pad(jnp.swapaxes(f, 0, 1), ((0, 0), (0, pad), (0, 0)))
    plain = lambda f: jnp.swapaxes(f[:, :C], 0, 1)
    flat = lambda a: a.reshape(-1, a.shape[-1])

    rows_a = passed_along(first_rows(emitted[0], row), "section", 1)
    rows_k = passed_along(first_rows(stash[0], row), "section", size // 2)
    rows_a, rows_k, emitted = lax.optimization_barrier((rows_a, rows_k, emitted))
    ahead = passed_along(emitted[0], "section", 1)
    rows_a, rows_k = exchanged(rows_a, S), exchanged(rows_k, S)

    ahead = lined(ahead)
    for l in range(L):
        mixed, _ = modes_forward(spec, l, rows_a, col, col_t, W)
        if l == 0:
            mixed, stash = lax.optimization_barrier((mixed, stash))
            kept = passed_along(stash[0], "section", size // 2)
        made = field_forward(ahead, flat(exchanged(mixed, S)), skip[l], up[l], down[l], back, row_t, W, l < L - 1)
        ahead = made[0]
        if l == 0:
            ahead, returned = lax.optimization_barrier((ahead, returned))
            top = passed_along(returned[0], "section", -1)
        if l < L - 1:
            rows_a = exchanged(made[1], S)
    sent = plain(ahead)

    kept = lined(kept)
    saved = []
    for l in range(L):
        mixed, modes = modes_forward(spec, l, rows_k, col, col_t, W)
        arrived = flat(exchanged(mixed, S))
        saved.append((kept, arrived, modes))
        if l < L - 1:
            kept, rows_k = field_forward(kept, arrived, skip[l], up[l], down[l], back, row_t, W, True)
            rows_k = exchanged(rows_k, S)
    g = lined(top)
    spec_grad = None
    skips, ups, downs = [], [], []
    for l in reversed(range(L)):
        v, arrived, modes = saved[l]
        gz, rows, gs, gu, gd = field_backward(v, g, arrived, skip[l], up[l], down[l], up_t[l], down_t[l], back, back_t, W)
        mixed, spec_grad = modes_backward(spec, l, exchanged(rows, S), modes, col, col_t, W, spec_grad)
        g = field_grad(g, gz, flat(exchanged(mixed, S)), skip_t[l], row)
        skips.insert(0, own_blocks(gs)[:C, :C])
        ups.insert(0, own_blocks(gu)[:, :C])
        downs.insert(0, own_blocks(gd)[:, :C].T)
    parts = [jnp.stack(skips), jnp.stack(ups), jnp.stack(downs)]
    flat_parts = jnp.concatenate([a.reshape(-1) for a in parts]) / W
    size_up = -(-flat_parts.size // 1024) * 1024
    packed = jnp.pad(flat_parts, (0, size_up - flat_parts.size)).reshape(1, -1, 128)
    everyone = lax.all_to_all(jnp.broadcast_to(packed, (S,) + packed.shape[1:]), "slab", 0, 0, tiled=True)
    total = jnp.sum(everyone, axis=0).reshape(-1)
    summed, at = [], 0
    for a in parts:
        summed.append(total[at:at + a.size].reshape(a.shape))
        at += a.size
    spec_grad = spec_grad.reshape(L, spec_w.shape[2], C, C, 2, spec_w.shape[6]).transpose(0, 1, 4, 2, 3, 5)
    return (sent[None], plain(g)[None], summed[0][None], summed[1][None], summed[2][None], spec_grad[None])


def work(*args):
    H = args[0].shape[2]
    K = args[6].shape[2]
    if H % 128 == 0 and K % 16 == 0 and H % HB == 0 and args[6].shape[6] == 128 and 2 * K * lax.axis_size("slab") == 128:
        return fast_shards(*args)
    return shards(*args)


def solution(mesh):
    placed = (
        P("section", None, "slab", None),
        P("section", None, "slab", None),
        P("section", None, "slab", None),
        P("section", None, None, None),
        P("section", None, None, None),
        P("section", None, None, None),
        P("section", None, "slab", None, None, None, None),
    )
    return jax.shard_map(
        work,
        mesh=mesh,
        in_specs=placed,
        out_specs=(
            P("section", None, "slab", None),
            P("section", None, "slab", None),
            P("section", None, None, None),
            P("section", None, None, None),
            P("section", None, None, None),
            P("section", None, "slab", None, None, None, None),
        ),
        check_vma=False,
    )
```
